32 devices in a mesh: dp: 4 (over x, y), x: 8 (over z, core).
Axes of the slice: x: 2, y: 2, z: 4, core: 2. Of those that a mesh axis runs over, the one named last changes fastest.
Arguments:
- start_pos: int32 [512], P('dp'), parts along dimension 0
- hidden_in: bfloat16 [4, 512, 2560], P(None, ('dp', 'x')), parts along dimension 1
- k_cache: bfloat16 [512, 256, 8, 128], P('dp', None, 'x'), parts along dimension 0
- v_cache: bfloat16 [512, 256, 8, 128], P('dp', None, 'x'), parts along dimension 0
- attn_norm: bfloat16 [2560], replicated
- w_q: bfloat16 [2560, 4096], replicated
- w_k: bfloat16 [2560, 1024], replicated
- w_v: bfloat16 [2560, 1024], replicated
- q_norm: bfloat16 [128], replicated
- k_norm: bfloat16 [128], replicated
- w_o: bfloat16 [4096, 2560], replicated
- mlp_norm: bfloat16 [2560], replicated
- w_gate: bfloat16 [2560, 9728], replicated
- w_up: bfloat16 [2560, 9728], replicated
- w_down: bfloat16 [9728, 2560], replicated
Outputs:
- output 1: bfloat16 [4, 512, 2560], P(None, ('dp', 'x')), parts along dimension 1
- output 2: bfloat16 [512, 256, 8, 128], P(('dp', 'x')), parts along dimension 0
- output 3: bfloat16 [512, 256, 8, 128], P(('dp', 'x')), parts along dimension 0
There are 4 independent parts. The reference program is written for one: setup_inputs(seed, part) draws one part's arguments, and reference() takes and returns one part's arrays. A program takes and returns all parts, laid end to end along the dimension named above; an argument that names none is the same for every part.
All inputs are finite; a program needn't handle non-finite values.
Results may differ from the reference program's by a relative error of at most 0.010418.
Values are sent between devices in bfloat16 or wider.
A program may use at most 1 GiB of HBM per device.

```python
import math
import jax
import jax.numpy as jnp
from jax import lax

BATCH = 128
T = 256
D = 2560
HEADS = 32
KV_HEADS = 8
HEAD = 128
FF = 9728
STEPS = 4

EPS = 1e-6
THETA = 1000000.0
Q_GAIN = math.sqrt(0.8 * math.log(T))
K_GAIN = math.sqrt(2.0 * math.log(T))


def rms_norm(values, gain_vec):
    values32 = values.astype(jnp.float32)
    inv_rms = lax.rsqrt(jnp.mean(values32 * values32, axis=-1, keepdims=True) + EPS)
    return values32 * inv_rms * gain_vec.astype(jnp.float32)


def rotary(values, positions):
    half_dim = HEAD // 2
    inv_freq = jnp.power(THETA, -jnp.arange(half_dim, dtype=jnp.float32) * 2.0 / HEAD)
    angles = positions.astype(jnp.float32)[..., None, None] * inv_freq
    cos_part = jnp.cos(angles)
    sin_part = jnp.sin(angles)
    first_half = values[..., :half_dim]
    second_half = values[..., half_dim:]
    return jnp.concatenate([first_half * cos_part - second_half * sin_part, second_half * cos_part + first_half * sin_part], axis=-1)


def setup_inputs(seed: int = 0, part: int = 0) -> dict:
    base_keys = jax.random.split(jax.random.key(seed), 16)

    def part_normal(index, shape):
        return jax.random.normal(jax.random.fold_in(base_keys[index], part), shape, jnp.float32)

    def shared_normal(index, shape):
        return jax.random.normal(base_keys[index], shape, jnp.float32)

    pos_key = jax.random.fold_in(base_keys[0], part)
    pos_draw = jax.random.randint(jax.random.fold_in(pos_key, 1), (BATCH,), T // 4, T - 3)
    top_row = jax.random.randint(jax.random.fold_in(pos_key, 2), (), 0, BATCH)
    start_pos = jnp.where(jnp.arange(BATCH) == top_row, T - 4, pos_draw).astype(jnp.int32)
    return dict(
        start_pos=start_pos,
        hidden_in=part_normal(1, (STEPS, BATCH, D)).astype(jnp.bfloat16),
        k_cache=part_normal(2, (BATCH, T, KV_HEADS, HEAD)).astype(jnp.bfloat16),
        v_cache=part_normal(3, (BATCH, T, KV_HEADS, HEAD)).astype(jnp.bfloat16),
        attn_norm=(1.0 + 0.2 * shared_normal(4, (D,))).astype(jnp.bfloat16),
        w_q=(shared_normal(5, (D, HEADS * HEAD)) * D ** -0.5).astype(jnp.bfloat16),
        w_k=(shared_normal(6, (D, KV_HEADS * HEAD)) * D ** -0.5).astype(jnp.bfloat16),
        w_v=(shared_normal(7, (D, KV_HEADS * HEAD)) * D ** -0.5).astype(jnp.bfloat16),
        q_norm=(Q_GAIN * (1.0 + 0.2 * shared_normal(8, (HEAD,)))).astype(jnp.bfloat16),
        k_norm=(K_GAIN * (1.0 + 0.2 * shared_normal(9, (HEAD,)))).astype(jnp.bfloat16),
        w_o=(shared_normal(10, (HEADS * HEAD, D)) * (HEADS * HEAD) ** -0.5).astype(jnp.bfloat16),
        mlp_norm=(1.0 + 0.2 * shared_normal(11, (D,))).astype(jnp.bfloat16),
        w_gate=(shared_normal(12, (D, FF)) * D ** -0.5).astype(jnp.bfloat16),
        w_up=(shared_normal(13, (D, FF)) * D ** -0.5).astype(jnp.bfloat16),
        w_down=(shared_normal(14, (FF, D)) * FF ** -0.5).astype(jnp.bfloat16),
    )


def reference(start_pos, hidden_in, k_cache, v_cache, attn_norm, w_q, w_k, w_v, q_norm, k_norm, w_o, mlp_norm, w_gate, w_up, w_down):
    group_size = HEADS // KV_HEADS
    score_scale = HEAD ** -0.5
    tokens = rms_norm(hidden_in, attn_norm).astype(jnp.bfloat16).reshape(STEPS * BATCH, D)
    queries = jnp.dot(tokens, w_q, preferred_element_type=jnp.float32).reshape(STEPS, BATCH, HEADS, HEAD)
    keys_new = jnp.dot(tokens, w_k, preferred_element_type=jnp.float32).reshape(STEPS, BATCH, KV_HEADS, HEAD)
    values_new = jnp.dot(tokens, w_v, preferred_element_type=jnp.float32).reshape(STEPS, BATCH, KV_HEADS, HEAD)
    positions = start_pos[None, :] + jnp.arange(STEPS)[:, None]
    queries = rotary(rms_norm(queries, q_norm), positions).astype(jnp.bfloat16)
    keys_new = rotary(rms_norm(keys_new, k_norm), positions).astype(jnp.bfloat16)
    values_new = values_new.astype(jnp.bfloat16)

    def one_row(row_inputs):
        row_q, row_k, row_v, row_kc, row_vc, row_pos = row_inputs

        def one_step(carry_in, step_inputs):
            cache_k, cache_v = carry_in
            step_q, step_k, step_v, slot_idx = step_inputs
            cache_k = lax.dynamic_update_slice(cache_k, step_k[None], (slot_idx, 0, 0))
            cache_v = lax.dynamic_update_slice(cache_v, step_v[None], (slot_idx, 0, 0))
            grouped = step_q.reshape(KV_HEADS, group_size, HEAD).astype(jnp.float32)
            scores = jnp.einsum('kgd,tkd->kgt', grouped, cache_k.astype(jnp.float32)) * score_scale
            slot_valid = jnp.arange(T) <= slot_idx
            scores = jnp.where(slot_valid, scores, -jnp.inf)
            weights = jnp.exp(scores - jnp.max(scores, axis=-1, keepdims=True))
            weight_sum = jnp.sum(weights, axis=-1)
            mixed_vals = jnp.einsum('kgt,tkd->kgd', weights.astype(jnp.bfloat16).astype(jnp.float32), cache_v.astype(jnp.float32))
            attended = (mixed_vals / weight_sum[..., None]).astype(jnp.bfloat16).reshape(HEADS * HEAD)
            return (cache_k, cache_v), attended

        (final_k, final_v), step_outs = lax.scan(one_step, (row_kc, row_vc), (row_q, row_k, row_v, row_pos + jnp.arange(STEPS)))
        return step_outs, final_k, final_v

    row_outs, k_out, v_out = lax.map(one_row, (jnp.swapaxes(queries, 0, 1), jnp.swapaxes(keys_new, 0, 1), jnp.swapaxes(values_new, 0, 1), k_cache, v_cache, start_pos))
    attended = jnp.swapaxes(row_outs, 0, 1).reshape(STEPS * BATCH, HEADS * HEAD)
    attn_out = jnp.dot(attended, w_o, preferred_element_type=jnp.float32).reshape(STEPS, BATCH, D)
    residual = (hidden_in.astype(jnp.float32) + attn_out).astype(jnp.bfloat16)
    normed = rms_norm(residual, mlp_norm).astype(jnp.bfloat16).reshape(STEPS * BATCH, D)
    gate_val = jnp.dot(normed, w_gate, preferred_element_type=jnp.float32)
    up_val = jnp.dot(normed, w_up, preferred_element_type=jnp.float32)
    activated = (jax.nn.silu(gate_val) * up_val).astype(jnp.bfloat16)
    down_val = jnp.dot(activated, w_down, preferred_element_type=jnp.float32).reshape(STEPS, BATCH, D)
    out_hidden = (residual.astype(jnp.float32) + down_val).astype(jnp.bfloat16)
    return (out_hidden, k_out, v_out)
```

```python
import jax
import jax.numpy as jnp
from jax import lax
from jax.experimental import pallas as pl
from jax.experimental.pallas import tpu as pltpu
from jax.sharding import PartitionSpec as P


EPS = 1e-6
THETA = 1000000.0
N_DEV = 8
CHUNKS = ((0, 6), (6, 12), (12, 16))


def rms_norm(values, gain_vec):
    values32 = values.astype(jnp.float32)
    inv_rms = lax.rsqrt(jnp.mean(values32 * values32, axis=-1, keepdims=True) + EPS)
    return values32 * inv_rms * gain_vec.astype(jnp.float32)


def rotary(values, positions):
    head_dim = values.shape[-1]
    half_dim = head_dim // 2
    inv_freq = jnp.power(THETA, -jnp.arange(half_dim, dtype=jnp.float32) * 2.0 / head_dim)
    angles = positions.astype(jnp.float32)[..., None, None] * inv_freq
    cos_part = jnp.cos(angles)
    sin_part = jnp.sin(angles)
    first_half = values[..., :half_dim]
    second_half = values[..., half_dim:]
    return jnp.concatenate([first_half * cos_part - second_half * sin_part, second_half * cos_part + first_half * sin_part], axis=-1)


def project(hidden, positions, attn_norm, w_q, w_k, w_v, q_norm, k_norm):
    n_steps, num_rows = hidden.shape[0], hidden.shape[1]
    head_dim = q_norm.shape[0]
    normed = rms_norm(hidden, attn_norm).astype(jnp.bfloat16)
    queries = jnp.einsum('sbd,de->sbe', normed, w_q, preferred_element_type=jnp.float32).reshape(n_steps, num_rows, -1, head_dim)
    keys_new = jnp.einsum('sbd,de->sbe', normed, w_k, preferred_element_type=jnp.float32).reshape(n_steps, num_rows, -1, head_dim)
    values_new = jnp.einsum('sbd,de->sbe', normed, w_v, preferred_element_type=jnp.float32).reshape(n_steps, num_rows, -1, head_dim)
    queries = rotary(rms_norm(queries, q_norm), positions).astype(jnp.bfloat16)
    keys_new = rotary(rms_norm(keys_new, k_norm), positions).astype(jnp.bfloat16)
    return queries, keys_new, values_new.astype(jnp.bfloat16)


def finish(hidden, attended, w_o, mlp_norm, w_gate, w_up, w_down):
    n_steps, num_rows = attended.shape[0], attended.shape[1]
    flat_attn = attended.reshape(n_steps, num_rows, -1)
    attn_out = jnp.einsum('sbe,ed->sbd', flat_attn, w_o, preferred_element_type=jnp.float32)
    residual = (hidden.astype(jnp.float32) + attn_out).astype(jnp.bfloat16)
    normed = rms_norm(residual, mlp_norm).astype(jnp.bfloat16)
    gate_val = jnp.einsum('sbd,df->sbf', normed, w_gate, preferred_element_type=jnp.float32)
    up_val = jnp.einsum('sbd,df->sbf', normed, w_up, preferred_element_type=jnp.float32)
    activated = (jax.nn.silu(gate_val) * up_val).astype(jnp.bfloat16)
    down_val = jnp.einsum('sbf,fd->sbd', activated, w_down, preferred_element_type=jnp.float32)
    return (residual.astype(jnp.float32) + down_val).astype(jnp.bfloat16)


NT = (((1,), (1,)), ((), ()))
NN = (((1,), (0,)), ((), ()))


def attend_one(pack, keys, values, pos):
    q = pack[:16]
    new_keys, new_values = pack[16:20], pack[20:24]
    scale = q.shape[-1] ** -0.5
    old = lax.dot_general(q, keys, NT, preferred_element_type=jnp.float32) * scale
    new = lax.dot_general(q, new_keys, NT, preferred_element_type=jnp.float32) * scale
    slot = lax.broadcasted_iota(jnp.int32, old.shape, 1)
    old = jnp.where(slot < pos, old, -jnp.inf)
    step = lax.broadcasted_iota(jnp.int32, new.shape, 0) // 4
    new = jnp.where(lax.broadcasted_iota(jnp.int32, new.shape, 1) <= step, new, -jnp.inf)
    peak = jnp.maximum(jnp.max(old, axis=-1, keepdims=True), jnp.max(new, axis=-1, keepdims=True))
    old_w, new_w = jnp.exp(old - peak), jnp.exp(new - peak)
    total = jnp.sum(old_w, axis=-1, keepdims=True) + jnp.sum(new_w, axis=-1, keepdims=True)
    mixed = lax.dot_general(old_w.astype(jnp.bfloat16), values, NN, preferred_element_type=jnp.float32)
    mixed = mixed + lax.dot_general(new_w.astype(jnp.bfloat16), new_values, NN, preferred_element_type=jnp.float32)
    return (mixed / total).astype(jnp.bfloat16)


def remote_attend(scalars, blocks, packs, offset):
    n_seq, num_slots, head_dim = blocks[0].shape[1:]

    def body(scal_ref, *refs):
        block_refs, pack_refs, out_refs = refs[:N_DEV], refs[N_DEV:2 * N_DEV], refs[2 * N_DEV:]
        seq = pl.program_id(0)
        me = scal_ref[128]
        for k in range(N_DEV):
            pos = scal_ref[(me ^ k) * 16 + offset + seq]
            out_refs[k][0] = attend_one(pack_refs[k][0], block_refs[k][0, 0], block_refs[k][1, 0], pos)

    return pl.pallas_call(
        body,
        grid_spec=pltpu.PrefetchScalarGridSpec(
            num_scalar_prefetch=1,
            grid=(n_seq,),
            in_specs=[pl.BlockSpec((2, 1, num_slots, head_dim), lambda i, s: (0, i, 0, 0))] * N_DEV
            + [pl.BlockSpec((1, 24, head_dim), lambda i, s: (i, 0, 0))] * N_DEV,
            out_specs=[pl.BlockSpec((1, 16, head_dim), lambda i, s: (i, 0, 0))] * N_DEV,
        ),
        out_shape=[jax.ShapeDtypeStruct((n_seq, 16, head_dim), jnp.bfloat16)] * N_DEV,
        cost_estimate=pl.CostEstimate(flops=n_seq * 40_000_000, bytes_accessed=n_seq * 1_100_000, transcendentals=0),
        name="remote_attend",
    )(scalars, *blocks, *packs)


def settle(scalars, blocks, new_keys, new_values, pack, caches, offset, num_seqs):
    n_seq, num_slots, head_dim = blocks[0].shape[1:]
    with_attn, in_place = pack is not None, caches is not None
    n_steps = new_keys.shape[1]

    def body(scal_ref, *refs):
        refs = list(refs)
        block_refs = [refs.pop(0) for _ in range(N_DEV)]
        new_refs = [refs.pop(0) for _ in range(2)]
        pack_ref = refs.pop(0) if with_attn else None
        if in_place:
            refs = refs[2:]
        cache_refs = [refs.pop(0) for _ in range(2)]
        out_ref = refs.pop(0) if with_attn else None
        spread_refs = refs
        me = scal_ref[128]
        pos = scal_ref[me * 16 + offset + pl.program_id(0)]
        for kind in range(2):
            spread = spread_refs[kind]
            for k in range(N_DEV):
                spread[pl.ds(me ^ k, num_slots, stride=N_DEV), :] = block_refs[k][kind, 0].astype(jnp.float32)
            cache_refs[kind][0] = spread[...].reshape(num_slots, N_DEV, head_dim).astype(jnp.bfloat16)
            for step in range(n_steps):
                cache_refs[kind][0, pos + step] = new_refs[kind][0, step]
        if with_attn:
            for k in range(N_DEV):
                out_ref[0, me ^ k] = attend_one(pack_ref[0, me ^ k], block_refs[k][0, 0], block_refs[k][1, 0], pos)

    cache_block = pl.BlockSpec((1, num_slots, N_DEV, head_dim), lambda i, s: (offset + i, 0, 0, 0))
    in_specs = [pl.BlockSpec((2, 1, num_slots, head_dim), lambda i, s: (0, i, 0, 0))] * N_DEV
    in_specs += [pl.BlockSpec((1, n_steps, N_DEV, head_dim), lambda i, s: (i, 0, 0, 0))] * 2
    args = [scalars, *blocks, new_keys, new_values]
    if with_attn:
        in_specs.append(pl.BlockSpec((1, N_DEV, 24, head_dim), lambda i, s: (i, 0, 0, 0)))
        args.append(pack)
    aliases = {}
    if in_place:
        aliases = {len(args): 0, len(args) + 1: 1}
        in_specs += [pl.BlockSpec(memory_space=pl.ANY)] * 2
        args += list(caches)
    cache_shape = jax.ShapeDtypeStruct((num_seqs, num_slots, N_DEV, head_dim), jnp.bfloat16)
    out_specs, out_shape = [cache_block] * 2, [cache_shape] * 2
    if with_attn:
        out_specs.append(pl.BlockSpec((1, N_DEV, 16, head_dim), lambda i, s: (i, 0, 0, 0)))
        out_shape.append(jax.ShapeDtypeStruct((n_seq, N_DEV, 16, head_dim), jnp.bfloat16))
    return pl.pallas_call(
        body,
        grid_spec=pltpu.PrefetchScalarGridSpec(
            num_scalar_prefetch=1,
            grid=(n_seq,),
            in_specs=in_specs,
            out_specs=out_specs,
            scratch_shapes=[pltpu.VMEM((num_slots * N_DEV, head_dim), jnp.float32)] * 2,
        ),
        out_shape=out_shape,
        input_output_aliases=aliases,
        cost_estimate=pl.CostEstimate(flops=n_seq * 60_000_000, bytes_accessed=n_seq * 2_200_000, transcendentals=0),
        name="settle",
    )(*args)


def solution(mesh):
    row_spec = P(None, ('dp', 'x'), None)
    cache_in = P('dp', None, 'x', None)
    cache_out = P(('dp', 'x'), None, None, None)

    def swap(value, k):
        if k == 0:
            return value
        return lax.ppermute(value, 'x', [(i, i ^ k) for i in range(N_DEV)])

    order = (2, 3, 1, 4, 5, 6, 7)

    def swap_all(values):
        got = {0: values[0]}
        for k in order:
            got[k] = swap(values[k], k)
        return [got[k] for k in range(N_DEV)]

    def local_run(start_pos, hidden_in, k_heads, v_heads, attn_norm, w_q, w_k, w_v, q_norm, k_norm, w_o, mlp_norm, w_gate, w_up, w_down):
        me = lax.axis_index('x')
        n_steps, num_rows = hidden_in.shape[:2]
        num_slots, head_dim = k_heads.shape[1], k_heads.shape[3]
        my_pos = lax.dynamic_slice_in_dim(start_pos, me * num_rows, num_rows)
        scalars = jnp.concatenate([start_pos, me[None].astype(jnp.int32)])
        partners = [me ^ k for k in range(N_DEV)]
        xor_heads = jnp.stack(partners)

        def pieces(caches, chunk):
            lo, hi = chunk
            keys, values = (c.reshape(N_DEV * num_rows, num_slots, head_dim) for c in caches)
            return [
                jnp.stack([lax.dynamic_slice_in_dim(c, p * num_rows + lo, hi - lo) for c in (keys, values)])
                for p in partners
            ]

        caches = (k_heads, v_heads)
        a, b, r = CHUNKS
        got_a = swap_all(pieces(caches, a))
        positions = my_pos[None, :] + jnp.arange(n_steps)[:, None]
        queries, keys_new, values_new = project(hidden_in, positions, attn_norm, w_q, w_k, w_v, q_norm, k_norm)
        q_rows = jnp.transpose(queries.reshape(n_steps, num_rows, N_DEV, -1, head_dim), (1, 2, 0, 3, 4)).reshape(num_rows, N_DEV, -1, head_dim)
        k_rows = jnp.transpose(keys_new, (1, 2, 0, 3))
        v_rows = jnp.transpose(values_new, (1, 2, 0, 3))
        pack = jnp.concatenate([q_rows, k_rows, v_rows], axis=2)
        knat, vnat = jnp.swapaxes(keys_new, 0, 1), jnp.swapaxes(values_new, 0, 1)
        pack_r = jnp.take(jnp.swapaxes(pack[r[0]:r[1]], 0, 1), xor_heads, axis=0)
        got_q = swap_all([pack_r[k] for k in range(N_DEV)])
        *caches, pack = lax.optimization_barrier((*caches, pack))
        got_b = swap_all(pieces(caches, b))
        blocks_r = pieces(caches, r)
        o_r = remote_attend(scalars, blocks_r, got_q, r[0])
        got_o = swap_all(o_r)
        blocks_r, _ = lax.optimization_barrier((blocks_r, o_r))
        got_r = swap_all(blocks_r)
        k_out, v_out, o_a = settle(scalars, got_a, knat[a[0]:a[1]], vnat[a[0]:a[1]], pack[a[0]:a[1]], None, a[0], num_rows)
        k_out, v_out, o_b = settle(scalars, got_b, knat[b[0]:b[1]], vnat[b[0]:b[1]], pack[b[0]:b[1]], (k_out, v_out), b[0], num_rows)
        o_r = jnp.swapaxes(jnp.take(jnp.stack(got_o), xor_heads, axis=0), 0, 1)
        attended = jnp.concatenate([o_a, o_b, o_r], axis=0).reshape(num_rows, N_DEV, n_steps, -1, head_dim)
        attended = jnp.transpose(attended, (2, 0, 1, 3, 4)).reshape(n_steps, num_rows, -1)
        out_hidden = finish(hidden_in, attended, w_o, mlp_norm, w_gate, w_up, w_down)
        k_out, v_out = settle(scalars, got_r, knat[r[0]:r[1]], vnat[r[0]:r[1]], None, (k_out, v_out), r[0], num_rows)
        return out_hidden, k_out, v_out

    return jax.shard_map(local_run, mesh=mesh, in_specs=(P('dp'), row_spec, cache_in, cache_in) + (P(),) * 11, out_specs=(row_spec, cache_out, cache_out), check_vma=False)
```

```python
import jax
import jax.numpy as jnp
from jax import lax
from jax.experimental import pallas as pl
from jax.experimental.pallas import tpu as pltpu
from jax.sharding import PartitionSpec as P


EPS = 1e-6
THETA = 1000000.0
N_DEV = 8
FIRST, LOCAL, LAST = 2, 8, 14


def rms_norm(values, gain_vec):
    values32 = values.astype(jnp.float32)
    inv_rms = lax.rsqrt(jnp.mean(values32 * values32, axis=-1, keepdims=True) + EPS)
    return values32 * inv_rms * gain_vec.astype(jnp.float32)


def rotary(values, positions):
    head_dim = values.shape[-1]
    half_dim = head_dim // 2
    inv_freq = jnp.power(THETA, -jnp.arange(half_dim, dtype=jnp.float32) * 2.0 / head_dim)
    angles = positions.astype(jnp.float32)[..., None, None] * inv_freq
    cos_part = jnp.cos(angles)
    sin_part = jnp.sin(angles)
    first_half = values[..., :half_dim]
    second_half = values[..., half_dim:]
    return jnp.concatenate([first_half * cos_part - second_half * sin_part, second_half * cos_part + first_half * sin_part], axis=-1)


def project(hidden, positions, attn_norm, w_q, w_k, w_v, q_norm, k_norm):
    n_steps, num_rows = hidden.shape[0], hidden.shape[1]
    head_dim = q_norm.shape[0]
    normed = rms_norm(hidden, attn_norm).astype(jnp.bfloat16)
    queries = jnp.einsum('sbd,de->sbe', normed, w_q, preferred_element_type=jnp.float32).reshape(n_steps, num_rows, -1, head_dim)
    keys_new = jnp.einsum('sbd,de->sbe', normed, w_k, preferred_element_type=jnp.float32).reshape(n_steps, num_rows, -1, head_dim)
    values_new = jnp.einsum('sbd,de->sbe', normed, w_v, preferred_element_type=jnp.float32).reshape(n_steps, num_rows, -1, head_dim)
    queries = rotary(rms_norm(queries, q_norm), positions).astype(jnp.bfloat16)
    keys_new = rotary(rms_norm(keys_new, k_norm), positions).astype(jnp.bfloat16)
    return queries, keys_new, values_new.astype(jnp.bfloat16)


def finish(hidden, attended, w_o, mlp_norm, w_gate, w_up, w_down):
    n_steps, num_rows = attended.shape[0], attended.shape[1]
    flat_attn = attended.reshape(n_steps, num_rows, -1)
    attn_out = jnp.einsum('sbe,ed->sbd', flat_attn, w_o, preferred_element_type=jnp.float32)
    residual = (hidden.astype(jnp.float32) + attn_out).astype(jnp.bfloat16)
    normed = rms_norm(residual, mlp_norm).astype(jnp.bfloat16)
    gate_val = jnp.einsum('sbd,df->sbf', normed, w_gate, preferred_element_type=jnp.float32)
    up_val = jnp.einsum('sbd,df->sbf', normed, w_up, preferred_element_type=jnp.float32)
    activated = (jax.nn.silu(gate_val) * up_val).astype(jnp.bfloat16)
    down_val = jnp.einsum('sbf,fd->sbd', activated, w_down, preferred_element_type=jnp.float32)
    return (residual.astype(jnp.float32) + down_val).astype(jnp.bfloat16)


NT = (((1,), (1,)), ((), ()))
NN = (((1,), (0,)), ((), ()))


def attend_one(pack, keys, values, pos):
    q = pack[:16]
    new_keys, new_values = pack[16:20], pack[20:24]
    scale = q.shape[-1] ** -0.5
    old = lax.dot_general(q, keys, NT, preferred_element_type=jnp.float32) * scale
    new = lax.dot_general(q, new_keys, NT, preferred_element_type=jnp.float32) * scale
    slot = lax.broadcasted_iota(jnp.int32, old.shape, 1)
    old = jnp.where(slot < pos, old, -jnp.inf)
    step = lax.broadcasted_iota(jnp.int32, new.shape, 0) // 4
    new = jnp.where(lax.broadcasted_iota(jnp.int32, new.shape, 1) <= step, new, -jnp.inf)
    peak = jnp.maximum(jnp.max(old, axis=-1, keepdims=True), jnp.max(new, axis=-1, keepdims=True))
    old_w, new_w = jnp.exp(old - peak), jnp.exp(new - peak)
    total = jnp.sum(old_w, axis=-1, keepdims=True) + jnp.sum(new_w, axis=-1, keepdims=True)
    mixed = lax.dot_general(old_w.astype(jnp.bfloat16), values, NN, preferred_element_type=jnp.float32)
    mixed = mixed + lax.dot_general(new_w.astype(jnp.bfloat16), new_values, NN, preferred_element_type=jnp.float32)
    return (mixed / total).astype(jnp.bfloat16)


def cache_specs(num_slots, head_dim, first_row):
    return pl.BlockSpec((1, num_slots, head_dim), lambda i, s: (first_row(s) + i, 0, 0))


def remote_attend(scalars, caches, packs, offset):
    n_seq = packs[0].shape[0]
    num_slots, head_dim = caches[0].shape[1:]

    def body(scal_ref, *refs):
        key_refs, value_refs = refs[:N_DEV], refs[N_DEV:2 * N_DEV]
        pack_refs, out_refs = refs[2 * N_DEV:3 * N_DEV], refs[3 * N_DEV:]
        seq = pl.program_id(0)
        me = scal_ref[128]
        for k in range(N_DEV):
            pos = scal_ref[(me ^ k) * 16 + offset + seq]
            out_refs[k][0] = attend_one(pack_refs[k][0], key_refs[k][0], value_refs[k][0], pos)

    rows = [cache_specs(num_slots, head_dim, lambda s, k=k: (s[128] ^ k) * 16 + offset) for k in range(N_DEV)]
    return pl.pallas_call(
        body,
        grid_spec=pltpu.PrefetchScalarGridSpec(
            num_scalar_prefetch=1,
            grid=(n_seq,),
            in_specs=rows + rows + [pl.BlockSpec((1, 24, head_dim), lambda i, s: (i, 0, 0))] * N_DEV,
            out_specs=[pl.BlockSpec((1, 16, head_dim), lambda i, s: (i, 0, 0))] * N_DEV,
        ),
        out_shape=[jax.ShapeDtypeStruct((n_seq, 16, head_dim), jnp.bfloat16)] * N_DEV,
        cost_estimate=pl.CostEstimate(flops=n_seq * 40_000_000, bytes_accessed=n_seq * 1_100_000, transcendentals=0),
        name="remote_attend",
    )(scalars, *[caches[0]] * N_DEV, *[caches[1]] * N_DEV, *packs)


def settle(scalars, own, blocks, new_keys, new_values, pack, caches, chunk, num_seqs):
    lo, hi = chunk
    num_slots, head_dim = own[0].shape[1:]
    with_attn, in_place = pack is not None, caches is not None
    n_steps = new_keys.shape[1]

    def body(scal_ref, *refs):
        refs = list(refs)
        own_refs = [refs.pop(0) for _ in range(2)]
        block_refs = [refs.pop(0) for _ in range(N_DEV - 1)]
        new_refs = [refs.pop(0) for _ in range(2)]
        pack_ref = refs.pop(0) if with_attn else None
        if in_place:
            refs = refs[2:]
        cache_refs = [refs.pop(0) for _ in range(2)]
        out_ref = refs.pop(0) if with_attn else None
        spread_refs = refs
        me = scal_ref[128]
        pos = scal_ref[me * 16 + lo + pl.program_id(0)]

        def block(k, kind):
            return own_refs[kind][0] if k == 0 else block_refs[k - 1][kind, 0]

        for kind in range(2):
            spread = spread_refs[kind]
            for k in range(N_DEV):
                spread[pl.ds(me ^ k, num_slots, stride=N_DEV), :] = block(k, kind).astype(jnp.float32)
            cache_refs[kind][0] = spread[...].reshape(num_slots, N_DEV, head_dim).astype(jnp.bfloat16)
            for step in range(n_steps):
                cache_refs[kind][0, pos + step] = new_refs[kind][0, step]
        if with_attn:
            for k in range(N_DEV):
                out_ref[0, me ^ k] = attend_one(pack_ref[0, me ^ k], block(k, 0), block(k, 1), pos)

    cache_block = pl.BlockSpec((1, num_slots, N_DEV, head_dim), lambda i, s: (lo + i, 0, 0, 0))
    in_specs = [cache_specs(num_slots, head_dim, lambda s: s[128] * 16 + lo)] * 2
    in_specs += [
        pl.BlockSpec((2, 1, num_slots, head_dim), lambda i, s, first=lo - first: (0, first + i, 0, 0))
        for first, _ in blocks
    ]
    in_specs += [pl.BlockSpec((1, n_steps, N_DEV, head_dim), lambda i, s: (lo + i, 0, 0, 0))] * 2
    args = [scalars, *own, *[b for _, b in blocks], new_keys, new_values]
    if with_attn:
        in_specs.append(pl.BlockSpec((1, N_DEV, 24, head_dim), lambda i, s: (lo + i, 0, 0, 0)))
        args.append(pack)
    aliases = {}
    if in_place:
        aliases = {len(args): 0, len(args) + 1: 1}
        in_specs += [pl.BlockSpec(memory_space=pl.ANY)] * 2
        args += list(caches)
    cache_shape = jax.ShapeDtypeStruct((num_seqs, num_slots, N_DEV, head_dim), jnp.bfloat16)
    out_specs, out_shape = [cache_block] * 2, [cache_shape] * 2
    if with_attn:
        out_specs.append(pl.BlockSpec((1, N_DEV, 16, head_dim), lambda i, s: (i, 0, 0, 0)))
        out_shape.append(jax.ShapeDtypeStruct((hi - lo, N_DEV, 16, head_dim), jnp.bfloat16))
    return pl.pallas_call(
        body,
        grid_spec=pltpu.PrefetchScalarGridSpec(
            num_scalar_prefetch=1,
            grid=(hi - lo,),
            in_specs=in_specs,
            out_specs=out_specs,
            scratch_shapes=[pltpu.VMEM((num_slots * N_DEV, head_dim), jnp.float32)] * 2,
        ),
        out_shape=out_shape,
        input_output_aliases=aliases,
        cost_estimate=pl.CostEstimate(flops=(hi - lo) * 60_000_000, bytes_accessed=(hi - lo) * 2_200_000, transcendentals=0),
        name="settle",
    )(*args)


def solution(mesh):
    row_spec = P(None, ('dp', 'x'), None)
    cache_in = P('dp', None, 'x', None)
    cache_out = P(('dp', 'x'), None, None, None)
    near, far = (2, 3, 1), (4, 5, 6, 7)

    def swap(value, k):
        return lax.ppermute(value, 'x', [(i, i ^ k) for i in range(N_DEV)])

    def local_run(start_pos, hidden_in, k_heads, v_heads, attn_norm, w_q, w_k, w_v, q_norm, k_norm, w_o, mlp_norm, w_gate, w_up, w_down):
        me = lax.axis_index('x')
        n_steps, num_rows = hidden_in.shape[:2]
        num_slots, head_dim = k_heads.shape[1], k_heads.shape[3]
        my_pos = lax.dynamic_slice_in_dim(start_pos, me * num_rows, num_rows)
        scalars = jnp.concatenate([start_pos, me[None].astype(jnp.int32)])
        xor_heads = me ^ jnp.arange(N_DEV)
        own = tuple(c.reshape(N_DEV * num_rows, num_slots, head_dim) for c in (k_heads, v_heads))

        def exchange(caches, lo, hi, partners):
            return {
                k: (lo, swap(jnp.stack([lax.dynamic_slice_in_dim(c, (me ^ k) * num_rows + lo, hi - lo) for c in caches]), k))
                for k in partners
            }

        def swap_small(values):
            got = {k: swap(values[k], k) for k in near + far}
            return [values[0]] + [got[k] for k in range(1, N_DEV)]

        def chosen(*parts):
            merged = {k: v for part in parts for k, v in part.items()}
            return [merged[k] for k in range(1, N_DEV)]

        far_first = exchange(own, 0, FIRST, far)
        positions = my_pos[None, :] + jnp.arange(n_steps)[:, None]
        queries, keys_new, values_new = project(hidden_in, positions, attn_norm, w_q, w_k, w_v, q_norm, k_norm)
        q_rows = jnp.transpose(queries.reshape(n_steps, num_rows, N_DEV, -1, head_dim), (1, 2, 0, 3, 4)).reshape(num_rows, N_DEV, -1, head_dim)
        k_rows = jnp.transpose(keys_new, (1, 2, 0, 3))
        v_rows = jnp.transpose(values_new, (1, 2, 0, 3))
        pack = jnp.concatenate([q_rows, k_rows, v_rows], axis=2)
        new = jnp.swapaxes(keys_new, 0, 1), jnp.swapaxes(values_new, 0, 1)
        pack_r = jnp.take(jnp.swapaxes(pack[LOCAL:], 0, 1), xor_heads, axis=0)
        got_q = swap_small([pack_r[k] for k in range(N_DEV)])
        *held, pack = lax.optimization_barrier((*own, pack))
        near_local = exchange(held, 0, LOCAL, near)
        far_local = exchange(held, FIRST, LOCAL, far)
        o_r = remote_attend(scalars, own, got_q, LOCAL)
        got_o = swap_small(o_r)
        *held, _ = lax.optimization_barrier((*held, o_r[0]))
        near_rest = exchange(held, LOCAL, num_rows, near)
        far_rest = exchange(held, LOCAL, LAST, far)
        far_last = exchange(held, LAST, num_rows, far)
        *caches, o_a = settle(scalars, own, chosen(near_local, far_first), *new, pack, None, (0, FIRST), num_rows)
        *caches, o_b = settle(scalars, own, chosen(near_local, far_local), *new, pack, caches, (FIRST, LOCAL), num_rows)
        o_r = jnp.swapaxes(jnp.take(jnp.stack(got_o), xor_heads, axis=0), 0, 1)
        attended = jnp.concatenate([o_a, o_b, o_r], axis=0).reshape(num_rows, N_DEV, n_steps, -1, head_dim)
        attended = jnp.transpose(attended, (2, 0, 1, 3, 4)).reshape(n_steps, num_rows, -1)
        out_hidden = finish(hidden_in, attended, w_o, mlp_norm, w_gate, w_up, w_down)
        caches = settle(scalars, own, chosen(near_rest, far_rest), *new, None, caches, (LOCAL, LAST), num_rows)
        caches = settle(scalars, own, chosen(near_rest, far_last), *new, None, caches, (LAST, num_rows), num_rows)
        return out_hidden, *caches

    return jax.shard_map(local_run, mesh=mesh, in_specs=(P('dp'), row_spec, cache_in, cache_in) + (P(),) * 11, out_specs=(row_spec, cache_out, cache_out), check_vma=False)
```

```python
import jax
import jax.numpy as jnp
from jax import lax
from jax.experimental import pallas as pl
from jax.experimental.pallas import tpu as pltpu
from jax.sharding import PartitionSpec as P


EPS = 1e-6
THETA = 1000000.0
N_DEV = 8
FIRST, MIDDLE, LOCAL, LAST = 3, 7, 11, 15
N_NEW = 4
MAIN = 248


def rms_norm(values, gain_vec):
    values32 = values.astype(jnp.float32)
    inv_rms = lax.rsqrt(jnp.mean(values32 * values32, axis=-1, keepdims=True) + EPS)
    return values32 * inv_rms * gain_vec.astype(jnp.float32)


def rotary(values, positions):
    head_dim = values.shape[-1]
    half_dim = head_dim // 2
    inv_freq = jnp.power(THETA, -jnp.arange(half_dim, dtype=jnp.float32) * 2.0 / head_dim)
    angles = positions.astype(jnp.float32)[..., None, None] * inv_freq
    cos_part = jnp.cos(angles)
    sin_part = jnp.sin(angles)
    first_half = values[..., :half_dim]
    second_half = values[..., half_dim:]
    return jnp.concatenate([first_half * cos_part - second_half * sin_part, second_half * cos_part + first_half * sin_part], axis=-1)


def project(hidden, positions, attn_norm, w_q, w_k, w_v, q_norm, k_norm):
    n_steps, num_rows = hidden.shape[0], hidden.shape[1]
    head_dim = q_norm.shape[0]
    normed = rms_norm(hidden, attn_norm).astype(jnp.bfloat16)
    queries = jnp.einsum('sbd,de->sbe', normed, w_q, preferred_element_type=jnp.float32).reshape(n_steps, num_rows, -1, head_dim)
    keys_new = jnp.einsum('sbd,de->sbe', normed, w_k, preferred_element_type=jnp.float32).reshape(n_steps, num_rows, -1, head_dim)
    values_new = jnp.einsum('sbd,de->sbe', normed, w_v, preferred_element_type=jnp.float32).reshape(n_steps, num_rows, -1, head_dim)
    queries = rotary(rms_norm(queries, q_norm), positions).astype(jnp.bfloat16)
    keys_new = rotary(rms_norm(keys_new, k_norm), positions).astype(jnp.bfloat16)
    return queries, keys_new, values_new.astype(jnp.bfloat16)


def finish(hidden, attended, w_o, mlp_norm, w_gate, w_up, w_down):
    n_steps, num_rows = attended.shape[0], attended.shape[1]
    flat_attn = attended.reshape(n_steps, num_rows, -1)
    attn_out = jnp.einsum('sbe,ed->sbd', flat_attn, w_o, preferred_element_type=jnp.float32)
    residual = (hidden.astype(jnp.float32) + attn_out).astype(jnp.bfloat16)
    normed = rms_norm(residual, mlp_norm).astype(jnp.bfloat16)
    gate_val = jnp.einsum('sbd,df->sbf', normed, w_gate, preferred_element_type=jnp.float32)
    up_val = jnp.einsum('sbd,df->sbf', normed, w_up, preferred_element_type=jnp.float32)
    activated = (jax.nn.silu(gate_val) * up_val).astype(jnp.bfloat16)
    down_val = jnp.einsum('sbf,fd->sbd', activated, w_down, preferred_element_type=jnp.float32)
    return (residual.astype(jnp.float32) + down_val).astype(jnp.bfloat16)


NT = (((1,), (1,)), ((), ()))
NN = (((1,), (0,)), ((), ()))


def attend_one(q, keys, values, extra_keys, extra_values, main_end, tail_end):
    scale = q.shape[-1] ** -0.5
    old = lax.dot_general(q, keys, NT, preferred_element_type=jnp.float32) * scale
    new = lax.dot_general(q, extra_keys, NT, preferred_element_type=jnp.float32) * scale
    old = jnp.where(lax.broadcasted_iota(jnp.int32, old.shape, 1) < main_end, old, -jnp.inf)
    column = lax.broadcasted_iota(jnp.int32, new.shape, 1)
    step = lax.broadcasted_iota(jnp.int32, new.shape, 0) // 4
    open_end = jnp.where(column < N_NEW, tail_end - MAIN, step + N_NEW + 1)
    new = jnp.where(column < open_end, new, -jnp.inf)
    peak = jnp.maximum(jnp.max(old, axis=-1, keepdims=True), jnp.max(new, axis=-1, keepdims=True))
    old_w, new_w = jnp.exp(old - peak), jnp.exp(new - peak)
    total = jnp.sum(old_w, axis=-1, keepdims=True) + jnp.sum(new_w, axis=-1, keepdims=True)
    mixed = lax.dot_general(old_w.astype(jnp.bfloat16), values, NN, preferred_element_type=jnp.float32)
    mixed = mixed + lax.dot_general(new_w.astype(jnp.bfloat16), extra_values, NN, preferred_element_type=jnp.float32)
    return (mixed / total).astype(jnp.bfloat16)


def attend_whole(pack, keys, values, pos):
    fresh = pack[16:].astype(jnp.float32)
    extra_keys = pltpu.roll(fresh, N_NEW, 0).astype(jnp.bfloat16)
    return attend_one(pack[:16], keys, values, extra_keys, pack[16:], pos, 0)


def attend_block(pack, block_ref, pos):
    fresh = pack[16:].astype(jnp.float32)
    tail = block_ref[2 * MAIN:, :].astype(jnp.float32)
    upper = lax.broadcasted_iota(jnp.int32, tail.shape, 0) < N_NEW
    extra_keys = jnp.where(upper, tail, pltpu.roll(fresh, N_NEW, 0)).astype(jnp.bfloat16)
    extra_values = jnp.where(upper, pltpu.roll(tail, N_NEW, 0), fresh).astype(jnp.bfloat16)
    keys, values = block_ref[:MAIN + 8, :], block_ref[MAIN:, :]
    return attend_one(pack[:16], keys, values, extra_keys, extra_values, jnp.minimum(pos, MAIN), pos)


def without_new(values, pos):
    values = values.astype(jnp.float32)
    slot = lax.broadcasted_iota(jnp.int32, values.shape, 0)
    return jnp.where(slot < pos, values, pltpu.roll(values, values.shape[0] - N_NEW, 0))


def cache_specs(num_slots, head_dim, first_row):
    return pl.BlockSpec((1, num_slots, head_dim), lambda i, s: (first_row(s) + i, 0, 0))


def pack_blocks(scalars, own, chunk, partners):
    lo, hi = chunk
    num_slots, head_dim = own[0].shape[1:]
    count = len(partners)

    def body(scal_ref, *refs):
        key_refs, value_refs, out_refs = refs[:count], refs[count:2 * count], refs[2 * count:]
        me = scal_ref[128]
        for j, k in enumerate(partners):
            pos = scal_ref[(me ^ k) * 16 + lo + pl.program_id(0)]
            keys, values = without_new(key_refs[j][0], pos), without_new(value_refs[j][0], pos)
            out_refs[j][0, :MAIN] = keys[:MAIN].astype(jnp.bfloat16)
            out_refs[j][0, MAIN:2 * MAIN] = values[:MAIN].astype(jnp.bfloat16)
            upper = lax.broadcasted_iota(jnp.int32, (8, head_dim), 0) < N_NEW
            tail = jnp.where(upper, keys[MAIN:], pltpu.roll(values[MAIN:], N_NEW, 0))
            out_refs[j][0, 2 * MAIN:] = tail.astype(jnp.bfloat16)

    rows = [cache_specs(num_slots, head_dim, lambda s, k=k: (s[128] ^ k) * 16 + lo) for k in partners]
    size = 2 * (num_slots - N_NEW)
    return pl.pallas_call(
        body,
        grid_spec=pltpu.PrefetchScalarGridSpec(
            num_scalar_prefetch=1,
            grid=(hi - lo,),
            in_specs=rows + rows,
            out_specs=[pl.BlockSpec((1, size, head_dim), lambda i, s: (i, 0, 0))] * count,
        ),
        out_shape=[jax.ShapeDtypeStruct((hi - lo, size, head_dim), jnp.bfloat16)] * count,
        cost_estimate=pl.CostEstimate(flops=(hi - lo) * count * 1_000_000, bytes_accessed=(hi - lo) * count * 260_000, transcendentals=0),
        name="pack_blocks",
    )(scalars, *[own[0]] * count, *[own[1]] * count)


def remote_attend(scalars, caches, packs, offset):
    n_seq = packs[0].shape[0]
    num_slots, head_dim = caches[0].shape[1:]

    def body(scal_ref, *refs):
        key_refs, value_refs = refs[:N_DEV], refs[N_DEV:2 * N_DEV]
        pack_refs, out_refs = refs[2 * N_DEV:3 * N_DEV], refs[3 * N_DEV:]
        seq = pl.program_id(0)
        me = scal_ref[128]
        for k in range(N_DEV):
            pos = scal_ref[(me ^ k) * 16 + offset + seq]
            out_refs[k][0] = attend_whole(pack_refs[k][0], key_refs[k][0], value_refs[k][0], pos)

    rows = [cache_specs(num_slots, head_dim, lambda s, k=k: (s[128] ^ k) * 16 + offset) for k in range(N_DEV)]
    return pl.pallas_call(
        body,
        grid_spec=pltpu.PrefetchScalarGridSpec(
            num_scalar_prefetch=1,
            grid=(n_seq,),
            in_specs=rows + rows + [pl.BlockSpec((1, 24, head_dim), lambda i, s: (i, 0, 0))] * N_DEV,
            out_specs=[pl.BlockSpec((1, 16, head_dim), lambda i, s: (i, 0, 0))] * N_DEV,
        ),
        out_shape=[jax.ShapeDtypeStruct((n_seq, 16, head_dim), jnp.bfloat16)] * N_DEV,
        cost_estimate=pl.CostEstimate(flops=n_seq * 40_000_000, bytes_accessed=n_seq * 1_100_000, transcendentals=0),
        name="remote_attend",
    )(scalars, *[caches[0]] * N_DEV, *[caches[1]] * N_DEV, *packs)


def settle(scalars, own, blocks, new_keys, new_values, pack, caches, chunk, num_seqs):
    lo, hi = chunk
    num_slots, head_dim = own[0].shape[1:]
    with_attn, in_place = pack is not None, caches is not None
    n_steps = new_keys.shape[1]

    def body(scal_ref, *refs):
        refs = list(refs)
        own_refs = [refs.pop(0) for _ in range(2)]
        block_refs = [refs.pop(0) for _ in range(N_DEV - 1)]
        new_refs = [refs.pop(0) for _ in range(2)]
        pack_ref = refs.pop(0) if with_attn else None
        if in_place:
            refs = refs[2:]
        cache_refs = [refs.pop(0) for _ in range(2)]
        out_ref = refs.pop(0) if with_attn else None
        spread_refs = refs
        me = scal_ref[128]
        pos = scal_ref[me * 16 + lo + pl.program_id(0)]

        for kind in range(2):
            spread = spread_refs[kind]
            for k in range(N_DEV):
                if k == 0:
                    kept = without_new(own_refs[kind][0], pos)
                    main, tail = kept[:MAIN], kept[MAIN:]
                else:
                    main = block_refs[k - 1][0, kind * MAIN:(kind + 1) * MAIN].astype(jnp.float32)
                    tail = block_refs[k - 1][0, 2 * MAIN:].astype(jnp.float32)
                    tail = tail if kind == 0 else pltpu.roll(tail, N_NEW, 0)
                spread[pl.ds(me ^ k, MAIN, stride=N_DEV), :] = main
                spread[pl.ds(MAIN * N_DEV + (me ^ k), N_NEW, stride=N_DEV), :] = tail[:N_NEW]
            fixed = num_slots // 4
            kept = spread[:fixed * N_DEV, :].reshape(fixed, N_DEV, head_dim)
            cache_refs[kind][0, :fixed] = kept.astype(jnp.bfloat16)
            shape = (num_slots - fixed, N_DEV, head_dim)
            before = spread[fixed * N_DEV:, :].reshape(shape)
            after = spread[(fixed - N_NEW) * N_DEV:(num_slots - N_NEW) * N_DEV, :].reshape(shape)
            slot = lax.broadcasted_iota(jnp.int32, shape, 0) + fixed
            cache_refs[kind][0, fixed:] = jnp.where(slot < pos, before, after).astype(jnp.bfloat16)
            for step in range(n_steps):
                cache_refs[kind][0, pos + step] = new_refs[kind][0, step]
        if with_attn:
            for k in range(N_DEV):
                pack = pack_ref[0, me ^ k]
                if k == 0:
                    out_ref[0, me ^ k] = attend_whole(pack, own_refs[0][0], own_refs[1][0], pos)
                else:
                    out_ref[0, me ^ k] = attend_block(pack, block_refs[k - 1].at[0], pos)

    cache_block = pl.BlockSpec((1, num_slots, N_DEV, head_dim), lambda i, s: (lo + i, 0, 0, 0))
    in_specs = [cache_specs(num_slots, head_dim, lambda s: s[128] * 16 + lo)] * 2
    in_specs += [
        pl.BlockSpec((1, 2 * (num_slots - N_NEW), head_dim), lambda i, s, first=lo - first: (first + i, 0, 0))
        for first, _ in blocks
    ]
    in_specs += [pl.BlockSpec((1, n_steps, N_DEV, head_dim), lambda i, s: (lo + i, 0, 0, 0))] * 2
    args = [scalars, *own, *[b for _, b in blocks], new_keys, new_values]
    if with_attn:
        in_specs.append(pl.BlockSpec((1, N_DEV, 24, head_dim), lambda i, s: (lo + i, 0, 0, 0)))
        args.append(pack)
    aliases = {}
    if in_place:
        aliases = {len(args): 0, len(args) + 1: 1}
        in_specs += [pl.BlockSpec(memory_space=pl.ANY)] * 2
        args += list(caches)
    cache_shape = jax.ShapeDtypeStruct((num_seqs, num_slots, N_DEV, head_dim), jnp.bfloat16)
    out_specs, out_shape = [cache_block] * 2, [cache_shape] * 2
    if with_attn:
        out_specs.append(pl.BlockSpec((1, N_DEV, 16, head_dim), lambda i, s: (i, 0, 0, 0)))
        out_shape.append(jax.ShapeDtypeStruct((hi - lo, N_DEV, 16, head_dim), jnp.bfloat16))
    return pl.pallas_call(
        body,
        grid_spec=pltpu.PrefetchScalarGridSpec(
            num_scalar_prefetch=1,
            grid=(hi - lo,),
            in_specs=in_specs,
            out_specs=out_specs,
            scratch_shapes=[pltpu.VMEM((num_slots * N_DEV, head_dim), jnp.float32)] * 2,
        ),
        out_shape=out_shape,
        input_output_aliases=aliases,
        cost_estimate=pl.CostEstimate(flops=(hi - lo) * 60_000_000, bytes_accessed=(hi - lo) * 2_200_000, transcendentals=0),
        name="settle",
    )(*args)


def solution(mesh):
    row_spec = P(None, ('dp', 'x'), None)
    cache_in = P('dp', None, 'x', None)
    cache_out = P(('dp', 'x'), None, None, None)
    near, far = (2, 3, 1), (6, 7, 4, 5)

    def swap(value, k):
        return lax.ppermute(value, 'x', [(i, i ^ k) for i in range(N_DEV)])

    def local_run(start_pos, hidden_in, k_heads, v_heads, attn_norm, w_q, w_k, w_v, q_norm, k_norm, w_o, mlp_norm, w_gate, w_up, w_down):
        me = lax.axis_index('x')
        n_steps, num_rows = hidden_in.shape[:2]
        num_slots, head_dim = k_heads.shape[1], k_heads.shape[3]
        my_pos = lax.dynamic_slice_in_dim(start_pos, me * num_rows, num_rows)
        scalars = jnp.concatenate([start_pos, me[None].astype(jnp.int32)])
        xor_heads = me ^ jnp.arange(N_DEV)
        own = tuple(c.reshape(N_DEV * num_rows, num_slots, head_dim) for c in (k_heads, v_heads))

        def exchange(packed, lo):
            return {k: (lo, swap(block, k)) for k, block in packed.items()}

        def packed(caches, lo, hi, partners):
            return dict(zip(partners, pack_blocks(scalars, caches, (lo, hi), partners)))

        def swap_small(values):
            got = {k: swap(values[k], k) for k in near + far}
            return [values[0]] + [got[k] for k in range(1, N_DEV)]

        def chosen(*parts):
            merged = {k: v for part in parts for k, v in part.items()}
            return [merged[k] for k in range(1, N_DEV)]

        blocks = packed(own, 0, FIRST, far)
        far_first = exchange(blocks, 0)
        positions = my_pos[None, :] + jnp.arange(n_steps)[:, None]
        queries, keys_new, values_new = project(hidden_in, positions, attn_norm, w_q, w_k, w_v, q_norm, k_norm)
        q_rows = jnp.transpose(queries.reshape(n_steps, num_rows, N_DEV, -1, head_dim), (1, 2, 0, 3, 4)).reshape(num_rows, N_DEV, -1, head_dim)
        k_rows = jnp.transpose(keys_new, (1, 2, 0, 3))
        v_rows = jnp.transpose(values_new, (1, 2, 0, 3))
        pack = jnp.concatenate([q_rows, k_rows, v_rows], axis=2)
        new = jnp.swapaxes(keys_new, 0, 1), jnp.swapaxes(values_new, 0, 1)
        pack_r = jnp.take(jnp.swapaxes(pack[LOCAL:], 0, 1), xor_heads, axis=0)
        got_q = swap_small([pack_r[k] for k in range(N_DEV)])
        near_blocks = packed(own, 0, LOCAL, near)
        middle_blocks = packed(own, FIRST, MIDDLE, far)
        local_blocks = packed(own, MIDDLE, LOCAL, far)
        near_local = exchange(near_blocks, 0)
        far_middle = exchange(middle_blocks, FIRST)
        far_local = exchange(local_blocks, MIDDLE)
        o_r = remote_attend(scalars, own, got_q, LOCAL)
        got_o = swap_small(o_r)
        near_blocks = packed(own, LOCAL, num_rows, near)
        rest_blocks = packed(own, LOCAL, LAST, far)
        last_blocks = packed(own, LAST, num_rows, far)
        near_rest = exchange(near_blocks, LOCAL)
        far_rest = exchange(rest_blocks, LOCAL)
        far_last = exchange(last_blocks, LAST)
        *caches, o_a = settle(scalars, own, chosen(near_local, far_first), *new, pack, None, (0, FIRST), num_rows)
        *caches, o_b = settle(scalars, own, chosen(near_local, far_middle), *new, pack, caches, (FIRST, MIDDLE), num_rows)
        *caches, o_c = settle(scalars, own, chosen(near_local, far_local), *new, pack, caches, (MIDDLE, LOCAL), num_rows)
        o_r = jnp.swapaxes(jnp.take(jnp.stack(got_o), xor_heads, axis=0), 0, 1)
        attended = jnp.concatenate([o_a, o_b, o_c, o_r], axis=0).reshape(num_rows, N_DEV, n_steps, -1, head_dim)
        attended = jnp.transpose(attended, (2, 0, 1, 3, 4)).reshape(n_steps, num_rows, -1)
        out_hidden = finish(hidden_in, attended, w_o, mlp_norm, w_gate, w_up, w_down)
        caches = settle(scalars, own, chosen(near_rest, far_rest), *new, None, caches, (LOCAL, LAST), num_rows)
        caches = settle(scalars, own, chosen(near_rest, far_last), *new, None, caches, (LAST, num_rows), num_rows)
        return out_hidden, *caches

    return jax.shard_map(local_run, mesh=mesh, in_specs=(P('dp'), row_spec, cache_in, cache_in) + (P(),) * 11, out_specs=(row_spec, cache_out, cache_out), check_vma=False)
```

```python
import jax
import jax.numpy as jnp
from jax import lax
from jax.experimental import pallas as pl
from jax.experimental.pallas import tpu as pltpu
from jax.sharding import PartitionSpec as P


EPS = 1e-6
THETA = 1000000.0
N_DEV = 8
FIRST, MIDDLE, LOCAL, LAST = 3, 8, 11, 15
N_NEW = 4


MAIN = 248


def rms_norm(values, gain_vec):
    values32 = values.astype(jnp.float32)
    inv_rms = lax.rsqrt(jnp.mean(values32 * values32, axis=-1, keepdims=True) + EPS)
    return values32 * inv_rms * gain_vec.astype(jnp.float32)


def rotary(values, positions):
    head_dim = values.shape[-1]
    half_dim = head_dim // 2
    inv_freq = jnp.power(THETA, -jnp.arange(half_dim, dtype=jnp.float32) * 2.0 / head_dim)
    angles = positions.astype(jnp.float32)[..., None, None] * inv_freq
    cos_part = jnp.cos(angles)
    sin_part = jnp.sin(angles)
    first_half = values[..., :half_dim]
    second_half = values[..., half_dim:]
    return jnp.concatenate([first_half * cos_part - second_half * sin_part, second_half * cos_part + first_half * sin_part], axis=-1)


def project(hidden, positions, attn_norm, w_q, w_k, w_v, q_norm, k_norm):
    n_steps, num_rows = hidden.shape[0], hidden.shape[1]
    head_dim = q_norm.shape[0]
    normed = rms_norm(hidden, attn_norm).astype(jnp.bfloat16)
    queries = jnp.einsum('sbd,de->sbe', normed, w_q, preferred_element_type=jnp.float32).reshape(n_steps, num_rows, -1, head_dim)
    keys_new = jnp.einsum('sbd,de->sbe', normed, w_k, preferred_element_type=jnp.float32).reshape(n_steps, num_rows, -1, head_dim)
    values_new = jnp.einsum('sbd,de->sbe', normed, w_v, preferred_element_type=jnp.float32).reshape(n_steps, num_rows, -1, head_dim)
    queries = rotary(rms_norm(queries, q_norm), positions).astype(jnp.bfloat16)
    keys_new = rotary(rms_norm(keys_new, k_norm), positions).astype(jnp.bfloat16)
    return queries, keys_new, values_new.astype(jnp.bfloat16)


def finish(hidden, attended, w_o, mlp_norm, w_gate, w_up, w_down):
    n_steps, num_rows = attended.shape[0], attended.shape[1]
    flat_attn = attended.reshape(n_steps, num_rows, -1)
    attn_out = jnp.einsum('sbe,ed->sbd', flat_attn, w_o, preferred_element_type=jnp.float32)
    residual = (hidden.astype(jnp.float32) + attn_out).astype(jnp.bfloat16)
    normed = rms_norm(residual, mlp_norm).astype(jnp.bfloat16)
    gate_val = jnp.einsum('sbd,df->sbf', normed, w_gate, preferred_element_type=jnp.float32)
    up_val = jnp.einsum('sbd,df->sbf', normed, w_up, preferred_element_type=jnp.float32)
    activated = (jax.nn.silu(gate_val) * up_val).astype(jnp.bfloat16)
    down_val = jnp.einsum('sbf,fd->sbd', activated, w_down, preferred_element_type=jnp.float32)
    return (residual.astype(jnp.float32) + down_val).astype(jnp.bfloat16)


NT = (((1,), (1,)), ((), ()))
NN = (((1,), (0,)), ((), ()))


def attend_one(q, keys, values, extra_keys, extra_values, main_end, tail_end):
    scale = q.shape[-1] ** -0.5
    old = lax.dot_general(q, keys, NT, preferred_element_type=jnp.float32) * scale
    new = lax.dot_general(q, extra_keys, NT, preferred_element_type=jnp.float32) * scale
    old = jnp.where(lax.broadcasted_iota(jnp.int32, old.shape, 1) < main_end, old, -jnp.inf)
    column = lax.broadcasted_iota(jnp.int32, new.shape, 1)
    step = lax.broadcasted_iota(jnp.int32, new.shape, 0) // 4
    open_end = jnp.where(column < N_NEW, tail_end - MAIN, step + N_NEW + 1)
    new = jnp.where(column < open_end, new, -jnp.inf)
    peak = jnp.maximum(jnp.max(old, axis=-1, keepdims=True), jnp.max(new, axis=-1, keepdims=True))
    old_w, new_w = jnp.exp(old - peak), jnp.exp(new - peak)
    total = jnp.sum(old_w, axis=-1, keepdims=True) + jnp.sum(new_w, axis=-1, keepdims=True)
    mixed = lax.dot_general(old_w.astype(jnp.bfloat16), values, NN, preferred_element_type=jnp.float32)
    mixed = mixed + lax.dot_general(new_w.astype(jnp.bfloat16), extra_values, NN, preferred_element_type=jnp.float32)
    return (mixed / total).astype(jnp.bfloat16)


def attend_whole(pack, keys, values, pos):
    fresh = pack[16:].astype(jnp.float32)
    extra_keys = pltpu.roll(fresh, N_NEW, 0).astype(jnp.bfloat16)
    return attend_one(pack[:16], keys, values, extra_keys, pack[16:], pos, 0)


def attend_block(pack, block_ref, pos):
    fresh = pack[16:].astype(jnp.float32)
    tail = block_ref[2 * MAIN:, :].astype(jnp.float32)
    upper = lax.broadcasted_iota(jnp.int32, tail.shape, 0) < N_NEW
    extra_keys = jnp.where(upper, tail, pltpu.roll(fresh, N_NEW, 0)).astype(jnp.bfloat16)
    extra_values = jnp.where(upper, pltpu.roll(tail, N_NEW, 0), fresh).astype(jnp.bfloat16)
    keys, values = block_ref[:MAIN + 8, :], block_ref[MAIN:, :]
    return attend_one(pack[:16], keys, values, extra_keys, extra_values, jnp.minimum(pos, MAIN), pos)


def without_new(values, pos):
    values = values.astype(jnp.float32)
    slot = lax.broadcasted_iota(jnp.int32, values.shape, 0)
    return jnp.where(slot < pos, values, pltpu.roll(values, values.shape[0] - N_NEW, 0))


def cache_specs(num_slots, head_dim, first_row):
    return pl.BlockSpec((1, num_slots, head_dim), lambda i, s, m: (first_row(m) + i, 0, 0))


def pack_blocks(scalars, own, chunk, partners):
    lo, hi = chunk
    num_slots, head_dim = own[0].shape[1:]
    count = len(partners)

    def body(scal_ref, me_ref, *refs):
        key_refs, value_refs, out_refs = refs[:count], refs[count:2 * count], refs[2 * count:]
        me = me_ref[0]
        for j, k in enumerate(partners):
            pos = scal_ref[(me ^ k) * 16 + lo + pl.program_id(0)]
            keys, values = without_new(key_refs[j][0], pos), without_new(value_refs[j][0], pos)
            out_refs[j][0, :MAIN] = keys[:MAIN].astype(jnp.bfloat16)
            out_refs[j][0, MAIN:2 * MAIN] = values[:MAIN].astype(jnp.bfloat16)
            upper = lax.broadcasted_iota(jnp.int32, (8, head_dim), 0) < N_NEW
            tail = jnp.where(upper, keys[MAIN:], pltpu.roll(values[MAIN:], N_NEW, 0))
            out_refs[j][0, 2 * MAIN:] = tail.astype(jnp.bfloat16)

    rows = [cache_specs(num_slots, head_dim, lambda m, k=k: (m[0] ^ k) * 16 + lo) for k in partners]
    size = 2 * (num_slots - N_NEW)
    return pl.pallas_call(
        body,
        grid_spec=pltpu.PrefetchScalarGridSpec(
            num_scalar_prefetch=2,
            grid=(hi - lo,),
            in_specs=rows + rows,
            out_specs=[pl.BlockSpec((1, size, head_dim), lambda i, s, m: (i, 0, 0))] * count,
        ),
        out_shape=[jax.ShapeDtypeStruct((hi - lo, size, head_dim), jnp.bfloat16)] * count,
        cost_estimate=pl.CostEstimate(flops=(hi - lo) * count * 1_000_000, bytes_accessed=(hi - lo) * count * 260_000, transcendentals=0),
        name="pack_blocks",
    )(*scalars, *[own[0]] * count, *[own[1]] * count)


def remote_attend(scalars, caches, packs, offset):
    n_seq = packs[0].shape[0]
    num_slots, head_dim = caches[0].shape[1:]

    def body(scal_ref, me_ref, *refs):
        key_refs, value_refs = refs[:N_DEV], refs[N_DEV:2 * N_DEV]
        pack_refs, out_refs = refs[2 * N_DEV:3 * N_DEV], refs[3 * N_DEV:]
        seq = pl.program_id(0)
        me = me_ref[0]
        for k in range(N_DEV):
            pos = scal_ref[(me ^ k) * 16 + offset + seq]
            out_refs[k][0] = attend_whole(pack_refs[k][0], key_refs[k][0], value_refs[k][0], pos)

    rows = [cache_specs(num_slots, head_dim, lambda m, k=k: (m[0] ^ k) * 16 + offset) for k in range(N_DEV)]
    return pl.pallas_call(
        body,
        grid_spec=pltpu.PrefetchScalarGridSpec(
            num_scalar_prefetch=2,
            grid=(n_seq,),
            in_specs=rows + rows + [pl.BlockSpec((1, 24, head_dim), lambda i, s, m: (i, 0, 0))] * N_DEV,
            out_specs=[pl.BlockSpec((1, 16, head_dim), lambda i, s, m: (i, 0, 0))] * N_DEV,
        ),
        out_shape=[jax.ShapeDtypeStruct((n_seq, 16, head_dim), jnp.bfloat16)] * N_DEV,
        cost_estimate=pl.CostEstimate(flops=n_seq * 40_000_000, bytes_accessed=n_seq * 1_100_000, transcendentals=0),
        name="remote_attend",
    )(*scalars, *[caches[0]] * N_DEV, *[caches[1]] * N_DEV, *packs)


def settle(scalars, own, blocks, new_keys, new_values, pack, caches, chunk, num_seqs):
    lo, hi = chunk
    num_slots, head_dim = own[0].shape[1:]
    with_attn, in_place = pack is not None, caches is not None
    n_steps = new_keys.shape[1]

    def body(scal_ref, me_ref, *refs):
        refs = list(refs)
        own_refs = [refs.pop(0) for _ in range(2)]
        block_refs = [refs.pop(0) for _ in range(N_DEV - 1)]
        new_refs = [refs.pop(0) for _ in range(2)]
        pack_ref = refs.pop(0) if with_attn else None
        if in_place:
            refs = refs[2:]
        cache_refs = [refs.pop(0) for _ in range(2)]
        out_ref = refs.pop(0) if with_attn else None
        spread_refs = refs
        me = me_ref[0]
        pos = scal_ref[me * 16 + lo + pl.program_id(0)]

        for kind in range(2):
            spread = spread_refs[kind]
            for k in range(N_DEV):
                if k == 0:
                    kept = without_new(own_refs[kind][0], pos)
                    main, tail = kept[:MAIN], kept[MAIN:]
                else:
                    main = block_refs[k - 1][0, kind * MAIN:(kind + 1) * MAIN].astype(jnp.float32)
                    tail = block_refs[k - 1][0, 2 * MAIN:].astype(jnp.float32)
                    tail = tail if kind == 0 else pltpu.roll(tail, N_NEW, 0)
                spread[pl.ds(me ^ k, MAIN, stride=N_DEV), :] = main
                spread[pl.ds(MAIN * N_DEV + (me ^ k), N_NEW, stride=N_DEV), :] = tail[:N_NEW]
            fixed = num_slots // 4
            kept = spread[:fixed * N_DEV, :].reshape(fixed, N_DEV, head_dim)
            cache_refs[kind][0, :fixed] = kept.astype(jnp.bfloat16)
            shape = (num_slots - fixed, N_DEV, head_dim)
            before = spread[fixed * N_DEV:, :].reshape(shape)
            after = spread[(fixed - N_NEW) * N_DEV:(num_slots - N_NEW) * N_DEV, :].reshape(shape)
            slot = lax.broadcasted_iota(jnp.int32, shape, 0) + fixed
            cache_refs[kind][0, fixed:] = jnp.where(slot < pos, before, after).astype(jnp.bfloat16)
            for step in range(n_steps):
                cache_refs[kind][0, pos + step] = new_refs[kind][0, step]
        if with_attn:
            for k in range(N_DEV):
                pack = pack_ref[0, me ^ k]
                if k == 0:
                    out_ref[0, me ^ k] = attend_whole(pack, own_refs[0][0], own_refs[1][0], pos)
                else:
                    out_ref[0, me ^ k] = attend_block(pack, block_refs[k - 1].at[0], pos)

    cache_block = pl.BlockSpec((1, num_slots, N_DEV, head_dim), lambda i, s, m: (lo + i, 0, 0, 0))
    in_specs = [cache_specs(num_slots, head_dim, lambda m: m[0] * 16 + lo)] * 2
    in_specs += [
        pl.BlockSpec((1, 2 * (num_slots - N_NEW), head_dim), lambda i, s, m, first=lo - first: (first + i, 0, 0))
        for first, _ in blocks
    ]
    in_specs += [pl.BlockSpec((1, n_steps, N_DEV, head_dim), lambda i, s, m: (lo + i, 0, 0, 0))] * 2
    args = [*scalars, *own, *[b for _, b in blocks], new_keys, new_values]
    if with_attn:
        in_specs.append(pl.BlockSpec((1, N_DEV, 24, head_dim), lambda i, s, m: (lo + i, 0, 0, 0)))
        args.append(pack)
    aliases = {}
    if in_place:
        aliases = {len(args): 0, len(args) + 1: 1}
        in_specs += [pl.BlockSpec(memory_space=pl.ANY)] * 2
        args += list(caches)
    cache_shape = jax.ShapeDtypeStruct((num_seqs, num_slots, N_DEV, head_dim), jnp.bfloat16)
    out_specs, out_shape = [cache_block] * 2, [cache_shape] * 2
    if with_attn:
        out_specs.append(pl.BlockSpec((1, N_DEV, 16, head_dim), lambda i, s, m: (i, 0, 0, 0)))
        out_shape.append(jax.ShapeDtypeStruct((hi - lo, N_DEV, 16, head_dim), jnp.bfloat16))
    return pl.pallas_call(
        body,
        grid_spec=pltpu.PrefetchScalarGridSpec(
            num_scalar_prefetch=2,
            grid=(hi - lo,),
            in_specs=in_specs,
            out_specs=out_specs,
            scratch_shapes=[pltpu.VMEM((num_slots * N_DEV, head_dim), jnp.float32)] * 2,
        ),
        out_shape=out_shape,
        input_output_aliases=aliases,
        cost_estimate=pl.CostEstimate(flops=(hi - lo) * 60_000_000, bytes_accessed=(hi - lo) * 2_200_000, transcendentals=0),
        name="settle",
    )(*args)


def solution(mesh):
    row_spec = P(None, ('dp', 'x'), None)
    cache_in = P('dp', None, 'x', None)
    cache_out = P(('dp', 'x'), None, None, None)
    near, far = (2, 3, 1), (6, 7, 4, 5)

    def swap(value, k):
        return lax.ppermute(value, 'x', [(i, i ^ k) for i in range(N_DEV)])

    def local_run(start_pos, hidden_in, k_heads, v_heads, attn_norm, w_q, w_k, w_v, q_norm, k_norm, w_o, mlp_norm, w_gate, w_up, w_down):
        me = lax.axis_index('x')
        n_steps, num_rows = hidden_in.shape[:2]
        num_slots, head_dim = k_heads.shape[1], k_heads.shape[3]
        my_pos = lax.dynamic_slice_in_dim(start_pos, me * num_rows, num_rows)
        scalars = start_pos, me[None].astype(jnp.int32)
        xor_heads = me ^ jnp.arange(N_DEV)
        own = tuple(c.reshape(N_DEV * num_rows, num_slots, head_dim) for c in (k_heads, v_heads))

        def exchange(packed, lo):
            return {k: (lo, swap(block, k)) for k, block in packed.items()}

        def packed(caches, lo, hi, partners):
            return dict(zip(partners, pack_blocks(scalars, caches, (lo, hi), partners)))

        def swap_small(values):
            got = {k: swap(values[k], k) for k in near + far}
            return [values[0]] + [got[k] for k in range(1, N_DEV)]

        def chosen(*parts):
            merged = {k: v for part in parts for k, v in part.items()}
            return [merged[k] for k in range(1, N_DEV)]

        far_first = {}
        for k in far:
            blocks = packed(own, 0, FIRST, (k,))
            far_first.update(exchange(blocks, 0))
        positions = my_pos[None, :] + jnp.arange(n_steps)[:, None]
        queries, keys_new, values_new = project(hidden_in, positions, attn_norm, w_q, w_k, w_v, q_norm, k_norm)
        q_rows = jnp.transpose(queries.reshape(n_steps, num_rows, N_DEV, -1, head_dim), (1, 2, 0, 3, 4)).reshape(num_rows, N_DEV, -1, head_dim)
        k_rows = jnp.transpose(keys_new, (1, 2, 0, 3))
        v_rows = jnp.transpose(values_new, (1, 2, 0, 3))
        pack = jnp.concatenate([q_rows, k_rows, v_rows], axis=2)
        new = jnp.swapaxes(keys_new, 0, 1), jnp.swapaxes(values_new, 0, 1)
        pack_r = jnp.take(jnp.swapaxes(pack[LOCAL:], 0, 1), xor_heads, axis=0)
        got_q = swap_small([pack_r[k] for k in range(N_DEV)])
        near_blocks = packed(own, 0, LOCAL, near)
        middle_blocks = packed(own, FIRST, MIDDLE, far)
        local_blocks = packed(own, MIDDLE, LOCAL, far)
        near_local = exchange(near_blocks, 0)
        far_middle = exchange(middle_blocks, FIRST)
        far_local = exchange(local_blocks, MIDDLE)
        o_r = remote_attend(scalars, own, got_q, LOCAL)
        got_o = swap_small(o_r)
        near_blocks = packed(own, LOCAL, num_rows, near)
        rest_blocks = packed(own, LOCAL, LAST, far)
        last_blocks = packed(own, LAST, num_rows, far)
        near_rest = exchange(near_blocks, LOCAL)
        far_rest = exchange(rest_blocks, LOCAL)
        far_last = exchange(last_blocks, LAST)
        *caches, o_a = settle(scalars, own, chosen(near_local, far_first), *new, pack, None, (0, FIRST), num_rows)
        *caches, o_b = settle(scalars, own, chosen(near_local, far_middle), *new, pack, caches, (FIRST, MIDDLE), num_rows)
        *caches, o_c = settle(scalars, own, chosen(near_local, far_local), *new, pack, caches, (MIDDLE, LOCAL), num_rows)
        o_r = jnp.swapaxes(jnp.take(jnp.stack(got_o), xor_heads, axis=0), 0, 1)
        attended = jnp.concatenate([o_a, o_b, o_c, o_r], axis=0).reshape(num_rows, N_DEV, n_steps, -1, head_dim)
        attended = jnp.transpose(attended, (2, 0, 1, 3, 4)).reshape(n_steps, num_rows, -1)
        out_hidden = finish(hidden_in, attended, w_o, mlp_norm, w_gate, w_up, w_down)
        caches = settle(scalars, own, chosen(near_rest, far_rest), *new, None, caches, (LOCAL, LAST), num_rows)
        caches = settle(scalars, own, chosen(near_rest, far_last), *new, None, caches, (LAST, num_rows), num_rows)
        return out_hidden, *caches

    return jax.shard_map(local_run, mesh=mesh, in_specs=(P('dp'), row_spec, cache_in, cache_in) + (P(),) * 11, out_specs=(row_spec, cache_out, cache_out), check_vma=False)
```

```python
import jax
import jax.numpy as jnp
from jax import lax
from jax.experimental import pallas as pl
from jax.experimental.pallas import tpu as pltpu
from jax.sharding import PartitionSpec as P


EPS = 1e-6
THETA = 1000000.0
N_DEV = 8
FIRST, MIDDLE, LOCAL, LAST = 3, 9, 11, 15
N_NEW = 4


MAIN = 248


def rms_norm(values, gain_vec):
    values32 = values.astype(jnp.float32)
    inv_rms = lax.rsqrt(jnp.mean(values32 * values32, axis=-1, keepdims=True) + EPS)
    return values32 * inv_rms * gain_vec.astype(jnp.float32)


def rotary(values, positions):
    head_dim = values.shape[-1]
    half_dim = head_dim // 2
    inv_freq = jnp.power(THETA, -jnp.arange(half_dim, dtype=jnp.float32) * 2.0 / head_dim)
    angles = positions.astype(jnp.float32)[..., None, None] * inv_freq
    cos_part = jnp.cos(angles)
    sin_part = jnp.sin(angles)
    first_half = values[..., :half_dim]
    second_half = values[..., half_dim:]
    return jnp.concatenate([first_half * cos_part - second_half * sin_part, second_half * cos_part + first_half * sin_part], axis=-1)


def project(hidden, positions, attn_norm, w_q, w_k, w_v, q_norm, k_norm):
    n_steps, num_rows = hidden.shape[0], hidden.shape[1]
    head_dim = q_norm.shape[0]
    normed = rms_norm(hidden, attn_norm).astype(jnp.bfloat16)
    queries = jnp.einsum('sbd,de->sbe', normed, w_q, preferred_element_type=jnp.float32).reshape(n_steps, num_rows, -1, head_dim)
    keys_new = jnp.einsum('sbd,de->sbe', normed, w_k, preferred_element_type=jnp.float32).reshape(n_steps, num_rows, -1, head_dim)
    values_new = jnp.einsum('sbd,de->sbe', normed, w_v, preferred_element_type=jnp.float32).reshape(n_steps, num_rows, -1, head_dim)
    queries = rotary(rms_norm(queries, q_norm), positions).astype(jnp.bfloat16)
    keys_new = rotary(rms_norm(keys_new, k_norm), positions).astype(jnp.bfloat16)
    return queries, keys_new, values_new.astype(jnp.bfloat16)


def finish(hidden, attended, w_o, mlp_norm, w_gate, w_up, w_down):
    n_steps, num_rows = attended.shape[0], attended.shape[1]
    flat_attn = attended.reshape(n_steps, num_rows, -1)
    attn_out = jnp.einsum('sbe,ed->sbd', flat_attn, w_o, preferred_element_type=jnp.float32)
    residual = (hidden.astype(jnp.float32) + attn_out).astype(jnp.bfloat16)
    normed = rms_norm(residual, mlp_norm).astype(jnp.bfloat16)
    gate_val = jnp.einsum('sbd,df->sbf', normed, w_gate, preferred_element_type=jnp.float32)
    up_val = jnp.einsum('sbd,df->sbf', normed, w_up, preferred_element_type=jnp.float32)
    activated = (jax.nn.silu(gate_val) * up_val).astype(jnp.bfloat16)
    down_val = jnp.einsum('sbf,fd->sbd', activated, w_down, preferred_element_type=jnp.float32)
    return (residual.astype(jnp.float32) + down_val).astype(jnp.bfloat16)


NT = (((1,), (1,)), ((), ()))
NN = (((1,), (0,)), ((), ()))


def attend_one(q, keys, values, extra_keys, extra_values, main_end, tail_end):
    scale = q.shape[-1] ** -0.5
    old = lax.dot_general(q, keys, NT, preferred_element_type=jnp.float32) * scale
    new = lax.dot_general(q, extra_keys, NT, preferred_element_type=jnp.float32) * scale
    old = jnp.where(lax.broadcasted_iota(jnp.int32, old.shape, 1) < main_end, old, -jnp.inf)
    column = lax.broadcasted_iota(jnp.int32, new.shape, 1)
    step = lax.broadcasted_iota(jnp.int32, new.shape, 0) // 4
    open_end = jnp.where(column < N_NEW, tail_end - MAIN, step + N_NEW + 1)
    new = jnp.where(column < open_end, new, -jnp.inf)
    peak = jnp.maximum(jnp.max(old, axis=-1, keepdims=True), jnp.max(new, axis=-1, keepdims=True))
    old_w, new_w = jnp.exp(old - peak), jnp.exp(new - peak)
    total = jnp.sum(old_w, axis=-1, keepdims=True) + jnp.sum(new_w, axis=-1, keepdims=True)
    mixed = lax.dot_general(old_w.astype(jnp.bfloat16), values, NN, preferred_element_type=jnp.float32)
    mixed = mixed + lax.dot_general(new_w.astype(jnp.bfloat16), extra_values, NN, preferred_element_type=jnp.float32)
    return (mixed / total).astype(jnp.bfloat16)


def attend_whole(pack, keys, values, pos):
    fresh = pack[16:].astype(jnp.float32)
    extra_keys = pltpu.roll(fresh, N_NEW, 0).astype(jnp.bfloat16)
    return attend_one(pack[:16], keys, values, extra_keys, pack[16:], pos, 0)


def attend_block(pack, block_ref, pos):
    fresh = pack[16:].astype(jnp.float32)
    tail = block_ref[2 * MAIN:, :].astype(jnp.float32)
    upper = lax.broadcasted_iota(jnp.int32, tail.shape, 0) < N_NEW
    extra_keys = jnp.where(upper, tail, pltpu.roll(fresh, N_NEW, 0)).astype(jnp.bfloat16)
    extra_values = jnp.where(upper, pltpu.roll(tail, N_NEW, 0), fresh).astype(jnp.bfloat16)
    keys, values = block_ref[:MAIN + 8, :], block_ref[MAIN:, :]
    return attend_one(pack[:16], keys, values, extra_keys, extra_values, jnp.minimum(pos, MAIN), pos)


def without_new(values, pos):
    values = values.astype(jnp.float32)
    slot = lax.broadcasted_iota(jnp.int32, values.shape, 0)
    return jnp.where(slot < pos, values, pltpu.roll(values, values.shape[0] - N_NEW, 0))


def cache_specs(num_slots, head_dim, first_row):
    return pl.BlockSpec((1, num_slots, head_dim), lambda i, s, m: (first_row(m) + i, 0, 0))


def pack_blocks(scalars, own, chunk, partners, group):
    lo, hi = chunk
    num_slots, head_dim = own[0].shape[1:]
    jobs = [(j, k, g) for j, k in enumerate(partners) for g in range(group)]

    def body(scal_ref, me_ref, *refs):
        key_refs, value_refs, out_refs = refs[:len(jobs)], refs[len(jobs):2 * len(jobs)], refs[2 * len(jobs):]
        me = me_ref[0]
        for (j, k, g), key_ref, value_ref in zip(jobs, key_refs, value_refs):
            pos = scal_ref[(me ^ k) * 16 + lo + pl.program_id(0) * group + g]
            keys, values = without_new(key_ref[0], pos), without_new(value_ref[0], pos)
            out_refs[j][g, :MAIN] = keys[:MAIN].astype(jnp.bfloat16)
            out_refs[j][g, MAIN:2 * MAIN] = values[:MAIN].astype(jnp.bfloat16)
            upper = lax.broadcasted_iota(jnp.int32, (8, head_dim), 0) < N_NEW
            tail = jnp.where(upper, keys[MAIN:], pltpu.roll(values[MAIN:], N_NEW, 0))
            out_refs[j][g, 2 * MAIN:] = tail.astype(jnp.bfloat16)

    rows = [
        pl.BlockSpec((1, num_slots, head_dim), lambda i, s, m, k=k, g=g: ((m[0] ^ k) * 16 + lo + i * group + g, 0, 0))
        for _, k, g in jobs
    ]
    size = 2 * (num_slots - N_NEW)
    return pl.pallas_call(
        body,
        grid_spec=pltpu.PrefetchScalarGridSpec(
            num_scalar_prefetch=2,
            grid=((hi - lo) // group,),
            in_specs=rows + rows,
            out_specs=[pl.BlockSpec((group, size, head_dim), lambda i, s, m: (i, 0, 0))] * len(partners),
        ),
        out_shape=[jax.ShapeDtypeStruct((hi - lo, size, head_dim), jnp.bfloat16)] * len(partners),
        cost_estimate=pl.CostEstimate(flops=(hi - lo) * len(partners) * 1_000_000, bytes_accessed=(hi - lo) * len(partners) * 260_000, transcendentals=0),
        name="pack_blocks",
    )(*scalars, *[own[0]] * len(jobs), *[own[1]] * len(jobs))


def remote_attend(scalars, caches, packs, offset):
    n_seq = packs[0].shape[0]
    num_slots, head_dim = caches[0].shape[1:]

    def body(scal_ref, me_ref, *refs):
        key_refs, value_refs = refs[:N_DEV], refs[N_DEV:2 * N_DEV]
        pack_refs, out_refs = refs[2 * N_DEV:3 * N_DEV], refs[3 * N_DEV:]
        seq = pl.program_id(0)
        me = me_ref[0]
        for k in range(N_DEV):
            pos = scal_ref[(me ^ k) * 16 + offset + seq]
            out_refs[k][0] = attend_whole(pack_refs[k][0], key_refs[k][0], value_refs[k][0], pos)

    rows = [cache_specs(num_slots, head_dim, lambda m, k=k: (m[0] ^ k) * 16 + offset) for k in range(N_DEV)]
    return pl.pallas_call(
        body,
        grid_spec=pltpu.PrefetchScalarGridSpec(
            num_scalar_prefetch=2,
            grid=(n_seq,),
            in_specs=rows + rows + [pl.BlockSpec((1, 24, head_dim), lambda i, s, m: (i, 0, 0))] * N_DEV,
            out_specs=[pl.BlockSpec((1, 16, head_dim), lambda i, s, m: (i, 0, 0))] * N_DEV,
        ),
        out_shape=[jax.ShapeDtypeStruct((n_seq, 16, head_dim), jnp.bfloat16)] * N_DEV,
        cost_estimate=pl.CostEstimate(flops=n_seq * 40_000_000, bytes_accessed=n_seq * 1_100_000, transcendentals=0),
        name="remote_attend",
    )(*scalars, *[caches[0]] * N_DEV, *[caches[1]] * N_DEV, *packs)


def settle(scalars, own, blocks, new_keys, new_values, pack, caches, chunk, num_seqs):
    lo, hi = chunk
    num_slots, head_dim = own[0].shape[1:]
    with_attn, in_place = pack is not None, caches is not None
    n_steps = new_keys.shape[1]

    def body(scal_ref, me_ref, *refs):
        refs = list(refs)
        own_refs = [refs.pop(0) for _ in range(2)]
        block_refs = [refs.pop(0) for _ in range(N_DEV - 1)]
        new_refs = [refs.pop(0) for _ in range(2)]
        pack_ref = refs.pop(0) if with_attn else None
        if in_place:
            refs = refs[2:]
        cache_refs = [refs.pop(0) for _ in range(2)]
        out_ref = refs.pop(0) if with_attn else None
        spread_refs = refs
        me = me_ref[0]
        pos = scal_ref[me * 16 + lo + pl.program_id(0)]

        for kind in range(2):
            spread = spread_refs[kind]
            for k in range(N_DEV):
                if k == 0:
                    kept = without_new(own_refs[kind][0], pos)
                    main, tail = kept[:MAIN], kept[MAIN:]
                else:
                    main = block_refs[k - 1][0, kind * MAIN:(kind + 1) * MAIN].astype(jnp.float32)
                    tail = block_refs[k - 1][0, 2 * MAIN:].astype(jnp.float32)
                    tail = tail if kind == 0 else pltpu.roll(tail, N_NEW, 0)
                spread[pl.ds(me ^ k, MAIN, stride=N_DEV), :] = main
                spread[pl.ds(MAIN * N_DEV + (me ^ k), N_NEW, stride=N_DEV), :] = tail[:N_NEW]
            fixed = num_slots // 4
            kept = spread[:fixed * N_DEV, :].reshape(fixed, N_DEV, head_dim)
            cache_refs[kind][0, :fixed] = kept.astype(jnp.bfloat16)
            shape = (num_slots - fixed, N_DEV, head_dim)
            before = spread[fixed * N_DEV:, :].reshape(shape)
            after = spread[(fixed - N_NEW) * N_DEV:(num_slots - N_NEW) * N_DEV, :].reshape(shape)
            slot = lax.broadcasted_iota(jnp.int32, shape, 0) + fixed
            cache_refs[kind][0, fixed:] = jnp.where(slot < pos, before, after).astype(jnp.bfloat16)
            for step in range(n_steps):
                cache_refs[kind][0, pos + step] = new_refs[kind][0, step]
        if with_attn:
            for k in range(N_DEV):
                pack = pack_ref[0, me ^ k]
                if k == 0:
                    out_ref[0, me ^ k] = attend_whole(pack, own_refs[0][0], own_refs[1][0], pos)
                else:
                    out_ref[0, me ^ k] = attend_block(pack, block_refs[k - 1].at[0], pos)

    cache_block = pl.BlockSpec((1, num_slots, N_DEV, head_dim), lambda i, s, m: (lo + i, 0, 0, 0))
    in_specs = [cache_specs(num_slots, head_dim, lambda m: m[0] * 16 + lo)] * 2
    in_specs += [
        pl.BlockSpec((1, 2 * (num_slots - N_NEW), head_dim), lambda i, s, m, first=lo - first: (first + i, 0, 0))
        for first, _ in blocks
    ]
    in_specs += [pl.BlockSpec((1, n_steps, N_DEV, head_dim), lambda i, s, m: (lo + i, 0, 0, 0))] * 2
    args = [*scalars, *own, *[b for _, b in blocks], new_keys, new_values]
    if with_attn:
        in_specs.append(pl.BlockSpec((1, N_DEV, 24, head_dim), lambda i, s, m: (lo + i, 0, 0, 0)))
        args.append(pack)
    aliases = {}
    if in_place:
        aliases = {len(args): 0, len(args) + 1: 1}
        in_specs += [pl.BlockSpec(memory_space=pl.ANY)] * 2
        args += list(caches)
    cache_shape = jax.ShapeDtypeStruct((num_seqs, num_slots, N_DEV, head_dim), jnp.bfloat16)
    out_specs, out_shape = [cache_block] * 2, [cache_shape] * 2
    if with_attn:
        out_specs.append(pl.BlockSpec((1, N_DEV, 16, head_dim), lambda i, s, m: (i, 0, 0, 0)))
        out_shape.append(jax.ShapeDtypeStruct((hi - lo, N_DEV, 16, head_dim), jnp.bfloat16))
    return pl.pallas_call(
        body,
        grid_spec=pltpu.PrefetchScalarGridSpec(
            num_scalar_prefetch=2,
            grid=(hi - lo,),
            in_specs=in_specs,
            out_specs=out_specs,
            scratch_shapes=[pltpu.VMEM((num_slots * N_DEV, head_dim), jnp.float32)] * 2,
        ),
        out_shape=out_shape,
        input_output_aliases=aliases,
        cost_estimate=pl.CostEstimate(flops=(hi - lo) * 60_000_000, bytes_accessed=(hi - lo) * 2_200_000, transcendentals=0),
        name="settle",
    )(*args)


def solution(mesh):
    row_spec = P(None, ('dp', 'x'), None)
    cache_in = P('dp', None, 'x', None)
    cache_out = P(('dp', 'x'), None, None, None)
    near, far = (2, 3, 1), (6, 7, 4, 5)

    def swap(value, k):
        return lax.ppermute(value, 'x', [(i, i ^ k) for i in range(N_DEV)])

    def local_run(start_pos, hidden_in, k_heads, v_heads, attn_norm, w_q, w_k, w_v, q_norm, k_norm, w_o, mlp_norm, w_gate, w_up, w_down):
        me = lax.axis_index('x')
        n_steps, num_rows = hidden_in.shape[:2]
        num_slots, head_dim = k_heads.shape[1], k_heads.shape[3]
        my_pos = lax.dynamic_slice_in_dim(start_pos, me * num_rows, num_rows)
        scalars = start_pos, me[None].astype(jnp.int32)
        xor_heads = me ^ jnp.arange(N_DEV)
        own = tuple(c.reshape(N_DEV * num_rows, num_slots, head_dim) for c in (k_heads, v_heads))

        def exchange(packed, lo):
            return {k: (lo, swap(block, k)) for k, block in packed.items()}

        def packed(caches, lo, hi, partners, group=1):
            return dict(zip(partners, pack_blocks(scalars, caches, (lo, hi), partners, group)))

        def swap_small(values):
            got = {k: swap(values[k], k) for k in near + far}
            return [values[0]] + [got[k] for k in range(1, N_DEV)]

        def chosen(*parts):
            merged = {k: v for part in parts for k, v in part.items()}
            return [merged[k] for k in range(1, N_DEV)]

        far_first = {}
        for k in far:
            blocks = packed(own, 0, FIRST, (k,), FIRST)
            far_first.update(exchange(blocks, 0))
        positions = my_pos[None, :] + jnp.arange(n_steps)[:, None]
        queries, keys_new, values_new = project(hidden_in, positions, attn_norm, w_q, w_k, w_v, q_norm, k_norm)
        q_rows = jnp.transpose(queries.reshape(n_steps, num_rows, N_DEV, -1, head_dim), (1, 2, 0, 3, 4)).reshape(num_rows, N_DEV, -1, head_dim)
        k_rows = jnp.transpose(keys_new, (1, 2, 0, 3))
        v_rows = jnp.transpose(values_new, (1, 2, 0, 3))
        pack = jnp.concatenate([q_rows, k_rows, v_rows], axis=2)
        new = jnp.swapaxes(keys_new, 0, 1), jnp.swapaxes(values_new, 0, 1)
        pack_r = jnp.take(jnp.swapaxes(pack[LOCAL:], 0, 1), xor_heads, axis=0)
        got_q = swap_small([pack_r[k] for k in range(N_DEV)])
        near_blocks = packed(own, 0, LOCAL, near)
        middle_blocks = packed(own, FIRST, MIDDLE, far)
        local_blocks = packed(own, MIDDLE, LOCAL, far)
        near_local = exchange(near_blocks, 0)
        far_middle = exchange(middle_blocks, FIRST)
        far_local = {}
        for k in far:
            far_local.update(exchange({k: local_blocks[k]}, MIDDLE))
        o_r = remote_attend(scalars, own, got_q, LOCAL)
        got_o = swap_small(o_r)
        near_blocks = packed(own, LOCAL, num_rows, near)
        rest_blocks = packed(own, LOCAL, LAST, far)
        last_blocks = packed(own, LAST, num_rows, far)
        near_rest = exchange(near_blocks, LOCAL)
        far_rest = {}
        for k in far:
            far_rest.update(exchange({k: rest_blocks[k]}, LOCAL))
        far_last = exchange(last_blocks, LAST)
        *caches, o_a = settle(scalars, own, chosen(near_local, far_first), *new, pack, None, (0, FIRST), num_rows)
        *caches, o_b = settle(scalars, own, chosen(near_local, far_middle), *new, pack, caches, (FIRST, MIDDLE), num_rows)
        *caches, o_c = settle(scalars, own, chosen(near_local, far_local), *new, pack, caches, (MIDDLE, LOCAL), num_rows)
        o_r = jnp.swapaxes(jnp.take(jnp.stack(got_o), xor_heads, axis=0), 0, 1)
        attended = jnp.concatenate([o_a, o_b, o_c, o_r], axis=0).reshape(num_rows, N_DEV, n_steps, -1, head_dim)
        attended = jnp.transpose(attended, (2, 0, 1, 3, 4)).reshape(n_steps, num_rows, -1)
        out_hidden = finish(hidden_in, attended, w_o, mlp_norm, w_gate, w_up, w_down)
        caches = settle(scalars, own, chosen(near_rest, far_rest), *new, None, caches, (LOCAL, LAST), num_rows)
        caches = settle(scalars, own, chosen(near_rest, far_last), *new, None, caches, (LAST, num_rows), num_rows)
        return out_hidden, *caches

    return jax.shard_map(local_run, mesh=mesh, in_specs=(P('dp'), row_spec, cache_in, cache_in) + (P(),) * 11, out_specs=(row_spec, cache_out, cache_out), check_vma=False)
```

```python
import jax
import jax.numpy as jnp
from jax import lax
from jax.experimental import pallas as pl
from jax.experimental.pallas import tpu as pltpu
from jax.sharding import PartitionSpec as P


EPS = 1e-6
THETA = 1000000.0
N_DEV = 8
FIRST, MIDDLE, LOCAL, LAST = 3, 8, 11, 15
N_NEW = 4


MAIN = 248


def rms_norm(values, gain_vec):
    values32 = values.astype(jnp.float32)
    inv_rms = lax.rsqrt(jnp.mean(values32 * values32, axis=-1, keepdims=True) + EPS)
    return values32 * inv_rms * gain_vec.astype(jnp.float32)


def rotary(values, positions):
    head_dim = values.shape[-1]
    half_dim = head_dim // 2
    inv_freq = jnp.power(THETA, -jnp.arange(half_dim, dtype=jnp.float32) * 2.0 / head_dim)
    angles = positions.astype(jnp.float32)[..., None, None] * inv_freq
    cos_part = jnp.cos(angles)
    sin_part = jnp.sin(angles)
    first_half = values[..., :half_dim]
    second_half = values[..., half_dim:]
    return jnp.concatenate([first_half * cos_part - second_half * sin_part, second_half * cos_part + first_half * sin_part], axis=-1)


def project(hidden, positions, attn_norm, w_q, w_k, w_v, q_norm, k_norm):
    n_steps, num_rows = hidden.shape[0], hidden.shape[1]
    head_dim = q_norm.shape[0]
    normed = rms_norm(hidden, attn_norm).astype(jnp.bfloat16)
    queries = jnp.einsum('sbd,de->sbe', normed, w_q, preferred_element_type=jnp.float32).reshape(n_steps, num_rows, -1, head_dim)
    keys_new = jnp.einsum('sbd,de->sbe', normed, w_k, preferred_element_type=jnp.float32).reshape(n_steps, num_rows, -1, head_dim)
    values_new = jnp.einsum('sbd,de->sbe', normed, w_v, preferred_element_type=jnp.float32).reshape(n_steps, num_rows, -1, head_dim)
    queries = rotary(rms_norm(queries, q_norm), positions).astype(jnp.bfloat16)
    keys_new = rotary(rms_norm(keys_new, k_norm), positions).astype(jnp.bfloat16)
    return queries, keys_new, values_new.astype(jnp.bfloat16)


def finish(hidden, attended, w_o, mlp_norm, w_gate, w_up, w_down):
    n_steps, num_rows = attended.shape[0], attended.shape[1]
    flat_attn = attended.reshape(n_steps, num_rows, -1)
    attn_out = jnp.einsum('sbe,ed->sbd', flat_attn, w_o, preferred_element_type=jnp.float32)
    residual = (hidden.astype(jnp.float32) + attn_out).astype(jnp.bfloat16)
    normed = rms_norm(residual, mlp_norm).astype(jnp.bfloat16)
    gate_val = jnp.einsum('sbd,df->sbf', normed, w_gate, preferred_element_type=jnp.float32)
    up_val = jnp.einsum('sbd,df->sbf', normed, w_up, preferred_element_type=jnp.float32)
    activated = (jax.nn.silu(gate_val) * up_val).astype(jnp.bfloat16)
    down_val = jnp.einsum('sbf,fd->sbd', activated, w_down, preferred_element_type=jnp.float32)
    return (residual.astype(jnp.float32) + down_val).astype(jnp.bfloat16)


NT = (((1,), (1,)), ((), ()))
NN = (((1,), (0,)), ((), ()))


def attend_one(q, keys, values, extra_keys, extra_values, main_end, tail_end):
    scale = q.shape[-1] ** -0.5
    old = lax.dot_general(q, keys, NT, preferred_element_type=jnp.float32) * scale
    new = lax.dot_general(q, extra_keys, NT, preferred_element_type=jnp.float32) * scale
    old = jnp.where(lax.broadcasted_iota(jnp.int32, old.shape, 1) < main_end, old, -jnp.inf)
    column = lax.broadcasted_iota(jnp.int32, new.shape, 1)
    step = lax.broadcasted_iota(jnp.int32, new.shape, 0) // 4
    open_end = jnp.where(column < N_NEW, tail_end - MAIN, step + N_NEW + 1)
    new = jnp.where(column < open_end, new, -jnp.inf)
    peak = jnp.maximum(jnp.max(old, axis=-1, keepdims=True), jnp.max(new, axis=-1, keepdims=True))
    old_w, new_w = jnp.exp(old - peak), jnp.exp(new - peak)
    total = jnp.sum(old_w, axis=-1, keepdims=True) + jnp.sum(new_w, axis=-1, keepdims=True)
    mixed = lax.dot_general(old_w.astype(jnp.bfloat16), values, NN, preferred_element_type=jnp.float32)
    mixed = mixed + lax.dot_general(new_w.astype(jnp.bfloat16), extra_values, NN, preferred_element_type=jnp.float32)
    return (mixed / total).astype(jnp.bfloat16)


def attend_whole(pack, keys, values, pos):
    fresh = pack[16:].astype(jnp.float32)
    extra_keys = pltpu.roll(fresh, N_NEW, 0).astype(jnp.bfloat16)
    return attend_one(pack[:16], keys, values, extra_keys, pack[16:], pos, 0)


def attend_block(pack, block_ref, pos):
    fresh = pack[16:].astype(jnp.float32)
    tail = block_ref[2 * MAIN:, :].astype(jnp.float32)
    upper = lax.broadcasted_iota(jnp.int32, tail.shape, 0) < N_NEW
    extra_keys = jnp.where(upper, tail, pltpu.roll(fresh, N_NEW, 0)).astype(jnp.bfloat16)
    extra_values = jnp.where(upper, pltpu.roll(tail, N_NEW, 0), fresh).astype(jnp.bfloat16)
    keys, values = block_ref[:MAIN + 8, :], block_ref[MAIN:, :]
    return attend_one(pack[:16], keys, values, extra_keys, extra_values, jnp.minimum(pos, MAIN), pos)


def without_new(values, pos):
    values = values.astype(jnp.float32)
    slot = lax.broadcasted_iota(jnp.int32, values.shape, 0)
    return jnp.where(slot < pos, values, pltpu.roll(values, values.shape[0] - N_NEW, 0))


def cache_specs(num_slots, head_dim, first_row):
    return pl.BlockSpec((1, num_slots, head_dim), lambda i, s, m: (first_row(m) + i, 0, 0))


def pack_blocks(scalars, own, chunk, partners, group):
    lo, hi = chunk
    num_slots, head_dim = own[0].shape[1:]
    jobs = [(j, k, g) for j, k in enumerate(partners) for g in range(group)]

    def body(scal_ref, me_ref, *refs):
        key_refs, value_refs, out_refs = refs[:len(jobs)], refs[len(jobs):2 * len(jobs)], refs[2 * len(jobs):]
        me = me_ref[0]
        for (j, k, g), key_ref, value_ref in zip(jobs, key_refs, value_refs):
            pos = scal_ref[(me ^ k) * 16 + lo + pl.program_id(0) * group + g]
            keys, values = without_new(key_ref[0], pos), without_new(value_ref[0], pos)
            out_refs[j][g, :MAIN] = keys[:MAIN].astype(jnp.bfloat16)
            out_refs[j][g, MAIN:2 * MAIN] = values[:MAIN].astype(jnp.bfloat16)
            upper = lax.broadcasted_iota(jnp.int32, (8, head_dim), 0) < N_NEW
            tail = jnp.where(upper, keys[MAIN:], pltpu.roll(values[MAIN:], N_NEW, 0))
            out_refs[j][g, 2 * MAIN:] = tail.astype(jnp.bfloat16)

    rows = [
        pl.BlockSpec((1, num_slots, head_dim), lambda i, s, m, k=k, g=g: ((m[0] ^ k) * 16 + lo + i * group + g, 0, 0))
        for _, k, g in jobs
    ]
    size = 2 * (num_slots - N_NEW)
    return pl.pallas_call(
        body,
        grid_spec=pltpu.PrefetchScalarGridSpec(
            num_scalar_prefetch=2,
            grid=((hi - lo) // group,),
            in_specs=rows + rows,
            out_specs=[pl.BlockSpec((group, size, head_dim), lambda i, s, m: (i, 0, 0))] * len(partners),
        ),
        out_shape=[jax.ShapeDtypeStruct((hi - lo, size, head_dim), jnp.bfloat16)] * len(partners),
        cost_estimate=pl.CostEstimate(flops=(hi - lo) * len(partners) * 1_000_000, bytes_accessed=(hi - lo) * len(partners) * 260_000, transcendentals=0),
        name="pack_blocks",
    )(*scalars, *[own[0]] * len(jobs), *[own[1]] * len(jobs))


def remote_attend(scalars, caches, packs, offset):
    n_seq = packs[0].shape[0]
    num_slots, head_dim = caches[0].shape[1:]

    def body(scal_ref, me_ref, *refs):
        key_refs, value_refs = refs[:N_DEV], refs[N_DEV:2 * N_DEV]
        pack_refs, out_refs = refs[2 * N_DEV:3 * N_DEV], refs[3 * N_DEV:]
        seq = pl.program_id(0)
        me = me_ref[0]
        for k in range(N_DEV):
            pos = scal_ref[(me ^ k) * 16 + offset + seq]
            out_refs[k][0] = attend_whole(pack_refs[k][0], key_refs[k][0], value_refs[k][0], pos)

    rows = [cache_specs(num_slots, head_dim, lambda m, k=k: (m[0] ^ k) * 16 + offset) for k in range(N_DEV)]
    return pl.pallas_call(
        body,
        grid_spec=pltpu.PrefetchScalarGridSpec(
            num_scalar_prefetch=2,
            grid=(n_seq,),
            in_specs=rows + rows + [pl.BlockSpec((1, 24, head_dim), lambda i, s, m: (i, 0, 0))] * N_DEV,
            out_specs=[pl.BlockSpec((1, 16, head_dim), lambda i, s, m: (i, 0, 0))] * N_DEV,
        ),
        out_shape=[jax.ShapeDtypeStruct((n_seq, 16, head_dim), jnp.bfloat16)] * N_DEV,
        cost_estimate=pl.CostEstimate(flops=n_seq * 40_000_000, bytes_accessed=n_seq * 1_100_000, transcendentals=0),
        name="remote_attend",
    )(*scalars, *[caches[0]] * N_DEV, *[caches[1]] * N_DEV, *packs)


def settle(scalars, own, blocks, new_keys, new_values, pack, caches, chunk, num_seqs):
    lo, hi = chunk
    num_slots, head_dim = own[0].shape[1:]
    with_attn, in_place = pack is not None, caches is not None
    n_steps = new_keys.shape[1]

    def body(scal_ref, me_ref, *refs):
        refs = list(refs)
        own_refs = [refs.pop(0) for _ in range(2)]
        block_refs = [refs.pop(0) for _ in range(N_DEV - 1)]
        new_refs = [refs.pop(0) for _ in range(2)]
        pack_ref = refs.pop(0) if with_attn else None
        if in_place:
            refs = refs[2:]
        cache_refs = [refs.pop(0) for _ in range(2)]
        out_ref = refs.pop(0) if with_attn else None
        spread_refs = refs
        me = me_ref[0]
        pos = scal_ref[me * 16 + lo + pl.program_id(0)]

        for kind in range(2):
            spread = spread_refs[kind]
            for k in range(N_DEV):
                if k == 0:
                    kept = without_new(own_refs[kind][0], pos)
                    main, tail = kept[:MAIN], kept[MAIN:]
                else:
                    main = block_refs[k - 1][0, kind * MAIN:(kind + 1) * MAIN].astype(jnp.float32)
                    tail = block_refs[k - 1][0, 2 * MAIN:].astype(jnp.float32)
                    tail = tail if kind == 0 else pltpu.roll(tail, N_NEW, 0)
                spread[pl.ds(me ^ k, MAIN, stride=N_DEV), :] = main
                spread[pl.ds(MAIN * N_DEV + (me ^ k), N_NEW, stride=N_DEV), :] = tail[:N_NEW]
            fixed = num_slots // 4
            kept = spread[:fixed * N_DEV, :].reshape(fixed, N_DEV, head_dim)
            cache_refs[kind][0, :fixed] = kept.astype(jnp.bfloat16)
            shape = (num_slots - fixed, N_DEV, head_dim)
            before = spread[fixed * N_DEV:, :].reshape(shape)
            after = spread[(fixed - N_NEW) * N_DEV:(num_slots - N_NEW) * N_DEV, :].reshape(shape)
            slot = lax.broadcasted_iota(jnp.int32, shape, 0) + fixed
            cache_refs[kind][0, fixed:] = jnp.where(slot < pos, before, after).astype(jnp.bfloat16)
            for step in range(n_steps):
                cache_refs[kind][0, pos + step] = new_refs[kind][0, step]
        if with_attn:
            for k in range(N_DEV):
                pack = pack_ref[0, me ^ k]
                if k == 0:
                    out_ref[0, me ^ k] = attend_whole(pack, own_refs[0][0], own_refs[1][0], pos)
                else:
                    out_ref[0, me ^ k] = attend_block(pack, block_refs[k - 1].at[0], pos)

    cache_block = pl.BlockSpec((1, num_slots, N_DEV, head_dim), lambda i, s, m: (lo + i, 0, 0, 0))
    in_specs = [cache_specs(num_slots, head_dim, lambda m: m[0] * 16 + lo)] * 2
    in_specs += [
        pl.BlockSpec((1, 2 * (num_slots - N_NEW), head_dim), lambda i, s, m, first=lo - first: (first + i, 0, 0))
        for first, _ in blocks
    ]
    in_specs += [pl.BlockSpec((1, n_steps, N_DEV, head_dim), lambda i, s, m: (lo + i, 0, 0, 0))] * 2
    args = [*scalars, *own, *[b for _, b in blocks], new_keys, new_values]
    if with_attn:
        in_specs.append(pl.BlockSpec((1, N_DEV, 24, head_dim), lambda i, s, m: (lo + i, 0, 0, 0)))
        args.append(pack)
    aliases = {}
    if in_place:
        aliases = {len(args): 0, len(args) + 1: 1}
        in_specs += [pl.BlockSpec(memory_space=pl.ANY)] * 2
        args += list(caches)
    cache_shape = jax.ShapeDtypeStruct((num_seqs, num_slots, N_DEV, head_dim), jnp.bfloat16)
    out_specs, out_shape = [cache_block] * 2, [cache_shape] * 2
    if with_attn:
        out_specs.append(pl.BlockSpec((1, N_DEV, 16, head_dim), lambda i, s, m: (i, 0, 0, 0)))
        out_shape.append(jax.ShapeDtypeStruct((hi - lo, N_DEV, 16, head_dim), jnp.bfloat16))
    return pl.pallas_call(
        body,
        grid_spec=pltpu.PrefetchScalarGridSpec(
            num_scalar_prefetch=2,
            grid=(hi - lo,),
            in_specs=in_specs,
            out_specs=out_specs,
            scratch_shapes=[pltpu.VMEM((num_slots * N_DEV, head_dim), jnp.float32)] * 2,
        ),
        out_shape=out_shape,
        input_output_aliases=aliases,
        cost_estimate=pl.CostEstimate(flops=(hi - lo) * 60_000_000, bytes_accessed=(hi - lo) * 2_200_000, transcendentals=0),
        name="settle",
    )(*args)


def merge(scalars, local, remote):
    num_rows = sum(part.shape[0] for part in local) + remote[0].shape[0]

    def body(me_ref, *refs):
        *parts, out_ref = refs
        row = 0
        for part in parts[:len(local)]:
            out_ref[row:row + part.shape[0]] = part[...]
            row += part.shape[0]
        for k, part in enumerate(parts[len(local):]):
            for seq in range(part.shape[0]):
                out_ref[row + seq, me_ref[0] ^ k] = part[seq]

    return pl.pallas_call(
        body,
        in_specs=[pl.BlockSpec(memory_space=pltpu.SMEM)] + [pl.BlockSpec(memory_space=pltpu.VMEM)] * (len(local) + N_DEV),
        out_specs=pl.BlockSpec(memory_space=pltpu.VMEM),
        out_shape=jax.ShapeDtypeStruct((num_rows,) + local[0].shape[1:], jnp.bfloat16),
        compiler_params=pltpu.CompilerParams(vmem_limit_bytes=8 << 20),
        cost_estimate=pl.CostEstimate(flops=1_000_000, bytes_accessed=1_000_000, transcendentals=0),
        name="merge",
    )(scalars[1], *local, *remote)


def solution(mesh):
    row_spec = P(None, ('dp', 'x'), None)
    cache_in = P('dp', None, 'x', None)
    cache_out = P(('dp', 'x'), None, None, None)
    near, far = (2, 3, 1), (6, 7, 4, 5)

    def swap(value, k):
        return lax.ppermute(value, 'x', [(i, i ^ k) for i in range(N_DEV)])

    def local_run(start_pos, hidden_in, k_heads, v_heads, attn_norm, w_q, w_k, w_v, q_norm, k_norm, w_o, mlp_norm, w_gate, w_up, w_down):
        me = lax.axis_index('x')
        n_steps, num_rows = hidden_in.shape[:2]
        num_slots, head_dim = k_heads.shape[1], k_heads.shape[3]
        my_pos = lax.dynamic_slice_in_dim(start_pos, me * num_rows, num_rows)
        scalars = start_pos, me[None].astype(jnp.int32)
        xor_heads = me ^ jnp.arange(N_DEV)
        own = tuple(c.reshape(N_DEV * num_rows, num_slots, head_dim) for c in (k_heads, v_heads))

        def exchange(packed, lo):
            return {k: (lo, swap(block, k)) for k, block in packed.items()}

        def packed(caches, lo, hi, partners, group=1):
            return dict(zip(partners, pack_blocks(scalars, caches, (lo, hi), partners, group)))

        def swap_small(values):
            got = {k: swap(values[k], k) for k in near + far}
            return [values[0]] + [got[k] for k in range(1, N_DEV)]

        def chosen(*parts):
            merged = {k: v for part in parts for k, v in part.items()}
            return [merged[k] for k in range(1, N_DEV)]

        far_first = {}
        for k in far:
            blocks = packed(own, 0, FIRST, (k,), FIRST)
            far_first.update(exchange(blocks, 0))
        positions = my_pos[None, :] + jnp.arange(n_steps)[:, None]
        queries, keys_new, values_new = project(hidden_in, positions, attn_norm, w_q, w_k, w_v, q_norm, k_norm)
        q_rows = jnp.transpose(queries.reshape(n_steps, num_rows, N_DEV, -1, head_dim), (1, 2, 0, 3, 4)).reshape(num_rows, N_DEV, -1, head_dim)
        k_rows = jnp.transpose(keys_new, (1, 2, 0, 3))
        v_rows = jnp.transpose(values_new, (1, 2, 0, 3))
        pack = jnp.concatenate([q_rows, k_rows, v_rows], axis=2)
        new = jnp.swapaxes(keys_new, 0, 1), jnp.swapaxes(values_new, 0, 1)
        pack_r = jnp.take(jnp.swapaxes(pack[LOCAL:], 0, 1), xor_heads, axis=0)
        got_q = swap_small([pack_r[k] for k in range(N_DEV)])
        near_blocks = packed(own, 0, LOCAL, near)
        middle_blocks = packed(own, FIRST, MIDDLE, far)
        local_blocks = packed(own, MIDDLE, LOCAL, far)
        near_local = exchange(near_blocks, 0)
        far_middle = exchange(middle_blocks, FIRST)
        far_local = {}
        for k in far:
            far_local.update(exchange({k: local_blocks[k]}, MIDDLE))
        o_r = remote_attend(scalars, own, got_q, LOCAL)
        got_o = swap_small(o_r)
        near_blocks = packed(own, LOCAL, num_rows, near)
        rest_blocks = packed(own, LOCAL, LAST, far)
        last_blocks = packed(own, LAST, num_rows, far)
        near_rest = exchange(near_blocks, LOCAL)
        far_last = exchange({far[0]: last_blocks[far[0]]}, LAST)
        far_rest = exchange(rest_blocks, LOCAL)
        far_last.update(exchange({k: last_blocks[k] for k in far[1:]}, LAST))
        *caches, o_a = settle(scalars, own, chosen(near_local, far_first), *new, pack, None, (0, FIRST), num_rows)
        *caches, o_b = settle(scalars, own, chosen(near_local, far_middle), *new, pack, caches, (FIRST, MIDDLE), num_rows)
        *caches, o_c = settle(scalars, own, chosen(near_local, far_local), *new, pack, caches, (MIDDLE, LOCAL), num_rows)
        attended = merge(scalars, (o_a, o_b, o_c), got_o).reshape(num_rows, N_DEV, n_steps, -1, head_dim)
        attended = jnp.transpose(attended, (2, 0, 1, 3, 4)).reshape(n_steps, num_rows, -1)
        out_hidden = finish(hidden_in, attended, w_o, mlp_norm, w_gate, w_up, w_down)
        caches = settle(scalars, own, chosen(near_rest, far_rest), *new, None, caches, (LOCAL, LAST), num_rows)
        caches = settle(scalars, own, chosen(near_rest, far_last), *new, None, caches, (LAST, num_rows), num_rows)
        return out_hidden, *caches

    return jax.shard_map(local_run, mesh=mesh, in_specs=(P('dp'), row_spec, cache_in, cache_in) + (P(),) * 11, out_specs=(row_spec, cache_out, cache_out), check_vma=False)
```

```python
import jax
import jax.numpy as jnp
from jax import lax
from jax.experimental import pallas as pl
from jax.experimental.pallas import tpu as pltpu
from jax.sharding import PartitionSpec as P


EPS = 1e-6
THETA = 1000000.0
N_DEV = 8
FIRST, MIDDLE, LOCAL, LAST = 3, 8, 11, 15
N_NEW = 4


MAIN = 248


def rms_norm(values, gain_vec):
    values32 = values.astype(jnp.float32)
    inv_rms = lax.rsqrt(jnp.mean(values32 * values32, axis=-1, keepdims=True) + EPS)
    return values32 * inv_rms * gain_vec.astype(jnp.float32)


def rotary(values, positions):
    head_dim = values.shape[-1]
    half_dim = head_dim // 2
    inv_freq = jnp.power(THETA, -jnp.arange(half_dim, dtype=jnp.float32) * 2.0 / head_dim)
    angles = positions.astype(jnp.float32)[..., None, None] * inv_freq
    cos_part = jnp.cos(angles)
    sin_part = jnp.sin(angles)
    first_half = values[..., :half_dim]
    second_half = values[..., half_dim:]
    return jnp.concatenate([first_half * cos_part - second_half * sin_part, second_half * cos_part + first_half * sin_part], axis=-1)


def project(hidden, positions, attn_norm, w_q, w_k, w_v, q_norm, k_norm):
    n_steps, num_rows = hidden.shape[0], hidden.shape[1]
    head_dim = q_norm.shape[0]
    normed = rms_norm(hidden, attn_norm).astype(jnp.bfloat16)
    queries = jnp.einsum('sbd,de->sbe', normed, w_q, preferred_element_type=jnp.float32).reshape(n_steps, num_rows, -1, head_dim)
    keys_new = jnp.einsum('sbd,de->sbe', normed, w_k, preferred_element_type=jnp.float32).reshape(n_steps, num_rows, -1, head_dim)
    values_new = jnp.einsum('sbd,de->sbe', normed, w_v, preferred_element_type=jnp.float32).reshape(n_steps, num_rows, -1, head_dim)
    queries = rotary(rms_norm(queries, q_norm), positions).astype(jnp.bfloat16)
    keys_new = rotary(rms_norm(keys_new, k_norm), positions).astype(jnp.bfloat16)
    return queries, keys_new, values_new.astype(jnp.bfloat16)


def finish(hidden, attended, w_o, mlp_norm, w_gate, w_up, w_down):
    n_steps, num_rows = attended.shape[0], attended.shape[1]
    flat_attn = attended.reshape(n_steps, num_rows, -1)
    attn_out = jnp.einsum('sbe,ed->sbd', flat_attn, w_o, preferred_element_type=jnp.float32)
    residual = (hidden.astype(jnp.float32) + attn_out).astype(jnp.bfloat16)
    normed = rms_norm(residual, mlp_norm).astype(jnp.bfloat16)
    gate_val = jnp.einsum('sbd,df->sbf', normed, w_gate, preferred_element_type=jnp.float32)
    up_val = jnp.einsum('sbd,df->sbf', normed, w_up, preferred_element_type=jnp.float32)
    activated = (jax.nn.silu(gate_val) * up_val).astype(jnp.bfloat16)
    down_val = jnp.einsum('sbf,fd->sbd', activated, w_down, preferred_element_type=jnp.float32)
    return (residual.astype(jnp.float32) + down_val).astype(jnp.bfloat16)


NT = (((1,), (1,)), ((), ()))
NN = (((1,), (0,)), ((), ()))


def attend_one(q, keys, values, extra_keys, extra_values, main_end, tail_end):
    scale = q.shape[-1] ** -0.5
    old = lax.dot_general(q, keys, NT, preferred_element_type=jnp.float32) * scale
    new = lax.dot_general(q, extra_keys, NT, preferred_element_type=jnp.float32) * scale
    old = jnp.where(lax.broadcasted_iota(jnp.int32, old.shape, 1) < main_end, old, -jnp.inf)
    column = lax.broadcasted_iota(jnp.int32, new.shape, 1)
    step = lax.broadcasted_iota(jnp.int32, new.shape, 0) // 4
    open_end = jnp.where(column < N_NEW, tail_end - MAIN, step + N_NEW + 1)
    new = jnp.where(column < open_end, new, -jnp.inf)
    peak = jnp.maximum(jnp.max(old, axis=-1, keepdims=True), jnp.max(new, axis=-1, keepdims=True))
    old_w, new_w = jnp.exp(old - peak), jnp.exp(new - peak)
    total = jnp.sum(old_w, axis=-1, keepdims=True) + jnp.sum(new_w, axis=-1, keepdims=True)
    mixed = lax.dot_general(old_w.astype(jnp.bfloat16), values, NN, preferred_element_type=jnp.float32)
    mixed = mixed + lax.dot_general(new_w.astype(jnp.bfloat16), extra_values, NN, preferred_element_type=jnp.float32)
    return (mixed / total).astype(jnp.bfloat16)


def attend_whole(pack, keys, values, pos):
    fresh = pack[16:].astype(jnp.float32)
    extra_keys = pltpu.roll(fresh, N_NEW, 0).astype(jnp.bfloat16)
    return attend_one(pack[:16], keys, values, extra_keys, pack[16:], pos, 0)


def attend_block(pack, block_ref, pos):
    fresh = pack[16:].astype(jnp.float32)
    tail = block_ref[2 * MAIN:, :].astype(jnp.float32)
    upper = lax.broadcasted_iota(jnp.int32, tail.shape, 0) < N_NEW
    extra_keys = jnp.where(upper, tail, pltpu.roll(fresh, N_NEW, 0)).astype(jnp.bfloat16)
    extra_values = jnp.where(upper, pltpu.roll(tail, N_NEW, 0), fresh).astype(jnp.bfloat16)
    keys, values = block_ref[:MAIN + 8, :], block_ref[MAIN:, :]
    return attend_one(pack[:16], keys, values, extra_keys, extra_values, jnp.minimum(pos, MAIN), pos)


def without_new(values, pos):
    values = values.astype(jnp.float32)
    slot = lax.broadcasted_iota(jnp.int32, values.shape, 0)
    return jnp.where(slot < pos, values, pltpu.roll(values, values.shape[0] - N_NEW, 0))


def cache_specs(num_slots, head_dim, first_row):
    return pl.BlockSpec((1, num_slots, head_dim), lambda i, s, m: (first_row(m) + i, 0, 0))


def pack_blocks(scalars, own, chunk, partners, group):
    lo, hi = chunk
    num_slots, head_dim = own[0].shape[1:]
    jobs = [(j, k, g) for j, k in enumerate(partners) for g in range(group)]

    def body(scal_ref, me_ref, *refs):
        key_refs, value_refs, out_refs = refs[:len(jobs)], refs[len(jobs):2 * len(jobs)], refs[2 * len(jobs):]
        me = me_ref[0]
        for (j, k, g), key_ref, value_ref in zip(jobs, key_refs, value_refs):
            pos = scal_ref[(me ^ k) * 16 + lo + pl.program_id(0) * group + g]
            keys, values = without_new(key_ref[0], pos), without_new(value_ref[0], pos)
            out_refs[j][g, :MAIN] = keys[:MAIN].astype(jnp.bfloat16)
            out_refs[j][g, MAIN:2 * MAIN] = values[:MAIN].astype(jnp.bfloat16)
            upper = lax.broadcasted_iota(jnp.int32, (8, head_dim), 0) < N_NEW
            tail = jnp.where(upper, keys[MAIN:], pltpu.roll(values[MAIN:], N_NEW, 0))
            out_refs[j][g, 2 * MAIN:] = tail.astype(jnp.bfloat16)

    rows = [
        pl.BlockSpec((1, num_slots, head_dim), lambda i, s, m, k=k, g=g: ((m[0] ^ k) * 16 + lo + i * group + g, 0, 0))
        for _, k, g in jobs
    ]
    size = 2 * (num_slots - N_NEW)
    return pl.pallas_call(
        body,
        grid_spec=pltpu.PrefetchScalarGridSpec(
            num_scalar_prefetch=2,
            grid=((hi - lo) // group,),
            in_specs=rows + rows,
            out_specs=[pl.BlockSpec((group, size, head_dim), lambda i, s, m: (i, 0, 0))] * len(partners),
        ),
        out_shape=[jax.ShapeDtypeStruct((hi - lo, size, head_dim), jnp.bfloat16)] * len(partners),
        cost_estimate=pl.CostEstimate(flops=(hi - lo) * len(partners) * 1_000_000, bytes_accessed=(hi - lo) * len(partners) * 260_000, transcendentals=0),
        name="pack_blocks",
    )(*scalars, *[own[0]] * len(jobs), *[own[1]] * len(jobs))


def remote_attend(scalars, caches, packs, offset):
    n_seq = packs[0].shape[0]
    num_slots, head_dim = caches[0].shape[1:]

    def body(scal_ref, me_ref, *refs):
        key_refs, value_refs = refs[:N_DEV], refs[N_DEV:2 * N_DEV]
        pack_refs, out_refs = refs[2 * N_DEV:3 * N_DEV], refs[3 * N_DEV:]
        seq = pl.program_id(0)
        me = me_ref[0]
        for k in range(N_DEV):
            pos = scal_ref[(me ^ k) * 16 + offset + seq]
            out_refs[k][0] = attend_whole(pack_refs[k][0], key_refs[k][0], value_refs[k][0], pos)

    rows = [cache_specs(num_slots, head_dim, lambda m, k=k: (m[0] ^ k) * 16 + offset) for k in range(N_DEV)]
    return pl.pallas_call(
        body,
        grid_spec=pltpu.PrefetchScalarGridSpec(
            num_scalar_prefetch=2,
            grid=(n_seq,),
            in_specs=rows + rows + [pl.BlockSpec((1, 24, head_dim), lambda i, s, m: (i, 0, 0))] * N_DEV,
            out_specs=[pl.BlockSpec((1, 16, head_dim), lambda i, s, m: (i, 0, 0))] * N_DEV,
        ),
        out_shape=[jax.ShapeDtypeStruct((n_seq, 16, head_dim), jnp.bfloat16)] * N_DEV,
        cost_estimate=pl.CostEstimate(flops=n_seq * 40_000_000, bytes_accessed=n_seq * 1_100_000, transcendentals=0),
        name="remote_attend",
    )(*scalars, *[caches[0]] * N_DEV, *[caches[1]] * N_DEV, *packs)


def settle(scalars, own, blocks, new_keys, new_values, pack, caches, chunk, num_seqs):
    lo, hi = chunk
    num_slots, head_dim = own[0].shape[1:]
    with_attn, in_place = pack is not None, caches is not None
    n_steps = new_keys.shape[1]

    def body(scal_ref, me_ref, *refs):
        refs = list(refs)
        own_refs = [refs.pop(0) for _ in range(2)]
        block_refs = [refs.pop(0) for _ in range(N_DEV - 1)]
        new_refs = [refs.pop(0) for _ in range(2)]
        pack_ref = refs.pop(0) if with_attn else None
        if in_place:
            refs = refs[2:]
        cache_refs = [refs.pop(0) for _ in range(2)]
        out_ref = refs.pop(0) if with_attn else None
        spread_refs = refs
        me = me_ref[0]
        pos = scal_ref[me * 16 + lo + pl.program_id(0)]

        for kind in range(2):
            spread = spread_refs[kind]
            for k in range(N_DEV):
                if k == 0:
                    kept = without_new(own_refs[kind][0], pos)
                    main, tail = kept[:MAIN], kept[MAIN:]
                else:
                    main = block_refs[k - 1][0, kind * MAIN:(kind + 1) * MAIN].astype(jnp.float32)
                    tail = block_refs[k - 1][0, 2 * MAIN:].astype(jnp.float32)
                    tail = tail if kind == 0 else pltpu.roll(tail, N_NEW, 0)
                spread[pl.ds(me ^ k, MAIN, stride=N_DEV), :] = main
                spread[pl.ds(MAIN * N_DEV + (me ^ k), N_NEW, stride=N_DEV), :] = tail[:N_NEW]
            fixed = num_slots // 4
            kept = spread[:fixed * N_DEV, :].reshape(fixed, N_DEV, head_dim)
            cache_refs[kind][0, :fixed] = kept.astype(jnp.bfloat16)
            shape = (num_slots - fixed, N_DEV, head_dim)
            before = spread[fixed * N_DEV:, :].reshape(shape)
            after = spread[(fixed - N_NEW) * N_DEV:(num_slots - N_NEW) * N_DEV, :].reshape(shape)
            slot = lax.broadcasted_iota(jnp.int32, shape, 0) + fixed
            cache_refs[kind][0, fixed:] = jnp.where(slot < pos, before, after).astype(jnp.bfloat16)
            for step in range(n_steps):
                cache_refs[kind][0, pos + step] = new_refs[kind][0, step]
        if with_attn:
            for k in range(N_DEV):
                pack = pack_ref[0, me ^ k]
                if k == 0:
                    out_ref[0, me ^ k] = attend_whole(pack, own_refs[0][0], own_refs[1][0], pos)
                else:
                    out_ref[0, me ^ k] = attend_block(pack, block_refs[k - 1].at[0], pos)

    cache_block = pl.BlockSpec((1, num_slots, N_DEV, head_dim), lambda i, s, m: (lo + i, 0, 0, 0))
    in_specs = [cache_specs(num_slots, head_dim, lambda m: m[0] * 16 + lo)] * 2
    in_specs += [
        pl.BlockSpec((1, 2 * (num_slots - N_NEW), head_dim), lambda i, s, m, first=lo - first: (first + i, 0, 0))
        for first, _ in blocks
    ]
    in_specs += [pl.BlockSpec((1, n_steps, N_DEV, head_dim), lambda i, s, m: (lo + i, 0, 0, 0))] * 2
    args = [*scalars, *own, *[b for _, b in blocks], new_keys, new_values]
    if with_attn:
        in_specs.append(pl.BlockSpec((1, N_DEV, 24, head_dim), lambda i, s, m: (lo + i, 0, 0, 0)))
        args.append(pack)
    aliases = {}
    if in_place:
        aliases = {len(args): 0, len(args) + 1: 1}
        in_specs += [pl.BlockSpec(memory_space=pl.ANY)] * 2
        args += list(caches)
    cache_shape = jax.ShapeDtypeStruct((num_seqs, num_slots, N_DEV, head_dim), jnp.bfloat16)
    out_specs, out_shape = [cache_block] * 2, [cache_shape] * 2
    if with_attn:
        out_specs.append(pl.BlockSpec((1, N_DEV, 16, head_dim), lambda i, s, m: (i, 0, 0, 0)))
        out_shape.append(jax.ShapeDtypeStruct((hi - lo, N_DEV, 16, head_dim), jnp.bfloat16))
    return pl.pallas_call(
        body,
        grid_spec=pltpu.PrefetchScalarGridSpec(
            num_scalar_prefetch=2,
            grid=(hi - lo,),
            in_specs=in_specs,
            out_specs=out_specs,
            scratch_shapes=[pltpu.VMEM((num_slots * N_DEV, head_dim), jnp.float32)] * 2,
        ),
        out_shape=out_shape,
        input_output_aliases=aliases,
        cost_estimate=pl.CostEstimate(flops=(hi - lo) * 60_000_000, bytes_accessed=(hi - lo) * 2_200_000, transcendentals=0),
        name="settle",
    )(*args)


def pack_first(start_pos, own, count, k):
    num_slots, head_dim = own[0].shape[1:]
    size = 2 * (num_slots - N_NEW)

    def body(pos_hbm, key_hbm, value_hbm, out_hbm, pos_smem, buf, out_buf, sems):
        row = (lax.axis_index('x') ^ k) * 16
        loads = [pltpu.make_async_copy(pos_hbm, pos_smem, sems.at[0])]
        loads += [pltpu.make_async_copy(src.at[pl.ds(row, count)], buf.at[i], sems.at[1 + i]) for i, src in enumerate((key_hbm, value_hbm))]
        for load in loads:
            load.start()
        for load in loads:
            load.wait()
        stores = []
        for g in range(count):
            pos = pos_smem[row + g]
            keys, values = without_new(buf[0, g], pos), without_new(buf[1, g], pos)
            out_buf[g, :MAIN] = keys[:MAIN].astype(jnp.bfloat16)
            out_buf[g, MAIN:2 * MAIN] = values[:MAIN].astype(jnp.bfloat16)
            upper = lax.broadcasted_iota(jnp.int32, (8, head_dim), 0) < N_NEW
            tail = jnp.where(upper, keys[MAIN:], pltpu.roll(values[MAIN:], N_NEW, 0))
            out_buf[g, 2 * MAIN:] = tail.astype(jnp.bfloat16)
            stores.append(pltpu.make_async_copy(out_buf.at[g], out_hbm.at[g], sems.at[3 + g]))
            stores[-1].start()
        for store in stores:
            store.wait()

    return pl.pallas_call(
        body,
        in_specs=[pl.BlockSpec(memory_space=pl.ANY)] * 3,
        out_specs=pl.BlockSpec(memory_space=pl.ANY),
        out_shape=jax.ShapeDtypeStruct((count, size, head_dim), jnp.bfloat16),
        scratch_shapes=[
            pltpu.SMEM(start_pos.shape, jnp.int32),
            pltpu.VMEM((2, count, num_slots, head_dim), jnp.bfloat16),
            pltpu.VMEM((count, size, head_dim), jnp.bfloat16),
            pltpu.SemaphoreType.DMA((3 + count,)),
        ],
        cost_estimate=pl.CostEstimate(flops=count * 1_000_000, bytes_accessed=count * 260_000, transcendentals=0),
        name="pack_first",
    )(start_pos, *own)


def settle_last(start_pos, own, blocks, new_keys, new_values, caches, seq):
    num_slots, head_dim = own[0].shape[1:]
    n_blocks, n_steps = len(blocks), new_keys.shape[1]

    def body(pos_hbm, *refs):
        refs = list(refs)
        own_refs = [refs.pop(0) for _ in range(2)]
        block_refs = [refs.pop(0) for _ in range(n_blocks)]
        new_refs = [refs.pop(0) for _ in range(2)]
        refs = refs[2:]
        cache_refs = [refs.pop(0) for _ in range(2)]
        pos_smem, own_buf, block_buf, new_buf, spread, out_buf, sems = refs
        me = lax.axis_index('x')
        loads = ([], [])
        for kind in range(2):
            def load(src, dst):
                loads[kind].append(pltpu.make_async_copy(src, dst, sems.at[kind, len(loads[kind])]))
                loads[kind][-1].start()

            load(own_refs[kind].at[me * 16 + seq], own_buf.at[kind])
            for j, (first, _) in enumerate(blocks):
                rows = pl.ds(kind * MAIN, MAIN)
                load(block_refs[j].at[seq - first, rows], block_buf.at[j, rows])
            if kind == 0:
                for j, (first, _) in enumerate(blocks):
                    rows = pl.ds(2 * MAIN, 2 * N_NEW)
                    load(block_refs[j].at[seq - first, rows], block_buf.at[j, rows])
                load(pos_hbm, pos_smem)
            load(new_refs[kind].at[seq], new_buf.at[kind])
        stores = []
        for kind in range(2):
            for copy in loads[kind]:
                copy.wait()
            pos = pos_smem[me * 16 + seq]
            for k in range(n_blocks + 1):
                if k == 0:
                    kept = without_new(own_buf[kind], pos)
                    main, tail = kept[:MAIN], kept[MAIN:]
                else:
                    main = block_buf[k - 1, kind * MAIN:(kind + 1) * MAIN].astype(jnp.float32)
                    tail = block_buf[k - 1, 2 * MAIN:].astype(jnp.float32)
                    tail = tail if kind == 0 else pltpu.roll(tail, N_NEW, 0)
                spread[kind, pl.ds(me ^ k, MAIN, stride=N_DEV), :] = main
                spread[kind, pl.ds(MAIN * N_DEV + (me ^ k), N_NEW, stride=N_DEV), :] = tail[:N_NEW]
            fixed = num_slots // 4
            kept = spread[kind, :fixed * N_DEV, :].reshape(fixed, N_DEV, head_dim)
            out_buf[kind, :fixed] = kept.astype(jnp.bfloat16)
            stores.append(pltpu.make_async_copy(out_buf.at[kind, :fixed], cache_refs[kind].at[seq, :fixed], sems.at[2, 2 + kind]))
            stores[-1].start()
            shape = (num_slots - fixed, N_DEV, head_dim)
            before = spread[kind, fixed * N_DEV:, :].reshape(shape)
            after = spread[kind, (fixed - N_NEW) * N_DEV:(num_slots - N_NEW) * N_DEV, :].reshape(shape)
            slot = lax.broadcasted_iota(jnp.int32, shape, 0) + fixed
            out_buf[kind, fixed:] = jnp.where(slot < pos, before, after).astype(jnp.bfloat16)
            for step in range(n_steps):
                out_buf[kind, pos + step] = new_buf[kind, step]
            stores.append(pltpu.make_async_copy(out_buf.at[kind, fixed:], cache_refs[kind].at[seq, fixed:], sems.at[2, kind]))
            stores[-1].start()
        for store in stores:
            store.wait()

    args = [start_pos, *own, *[b for _, b in blocks], new_keys, new_values, *caches]
    return pl.pallas_call(
        body,
        in_specs=[pl.BlockSpec(memory_space=pl.ANY)] * len(args),
        out_specs=[pl.BlockSpec(memory_space=pl.ANY)] * 2,
        out_shape=[jax.ShapeDtypeStruct(c.shape, c.dtype) for c in caches],
        input_output_aliases={len(args) - 2: 0, len(args) - 1: 1},
        scratch_shapes=[
            pltpu.SMEM(start_pos.shape, jnp.int32),
            pltpu.VMEM((2, num_slots, head_dim), jnp.bfloat16),
            pltpu.VMEM((n_blocks, 2 * (num_slots - N_NEW), head_dim), jnp.bfloat16),
            pltpu.VMEM((2, n_steps, N_DEV, head_dim), jnp.bfloat16),
            pltpu.VMEM((2, num_slots * N_DEV, head_dim), jnp.float32),
            pltpu.VMEM((2, num_slots, N_DEV, head_dim), jnp.bfloat16),
            pltpu.SemaphoreType.DMA((3, 2 * n_blocks + 4)),
        ],
        cost_estimate=pl.CostEstimate(flops=60_000_000, bytes_accessed=2_200_000, transcendentals=0),
        name="settle_last",
    )(*args)


def merge(scalars, local, remote):
    num_rows = sum(part.shape[0] for part in local) + remote[0].shape[0]

    def body(me_ref, *refs):
        *parts, out_ref = refs
        row = 0
        for part in parts[:len(local)]:
            out_ref[row:row + part.shape[0]] = part[...]
            row += part.shape[0]
        for k, part in enumerate(parts[len(local):]):
            for seq in range(part.shape[0]):
                out_ref[row + seq, me_ref[0] ^ k] = part[seq]

    return pl.pallas_call(
        body,
        in_specs=[pl.BlockSpec(memory_space=pltpu.SMEM)] + [pl.BlockSpec(memory_space=pltpu.VMEM)] * (len(local) + N_DEV),
        out_specs=pl.BlockSpec(memory_space=pltpu.VMEM),
        out_shape=jax.ShapeDtypeStruct((num_rows,) + local[0].shape[1:], jnp.bfloat16),
        compiler_params=pltpu.CompilerParams(vmem_limit_bytes=8 << 20),
        cost_estimate=pl.CostEstimate(flops=1_000_000, bytes_accessed=1_000_000, transcendentals=0),
        name="merge",
    )(scalars[1], *local, *remote)


def solution(mesh):
    row_spec = P(None, ('dp', 'x'), None)
    cache_in = P('dp', None, 'x', None)
    cache_out = P(('dp', 'x'), None, None, None)
    near, far = (2, 3, 1), (6, 7, 4, 5)

    def swap(value, k):
        return lax.ppermute(value, 'x', [(i, i ^ k) for i in range(N_DEV)])

    def local_run(start_pos, hidden_in, k_heads, v_heads, attn_norm, w_q, w_k, w_v, q_norm, k_norm, w_o, mlp_norm, w_gate, w_up, w_down):
        me = lax.axis_index('x')
        n_steps, num_rows = hidden_in.shape[:2]
        num_slots, head_dim = k_heads.shape[1], k_heads.shape[3]
        my_pos = lax.dynamic_slice_in_dim(start_pos, me * num_rows, num_rows)
        scalars = start_pos, me[None].astype(jnp.int32)
        xor_heads = me ^ jnp.arange(N_DEV)
        own = tuple(c.reshape(N_DEV * num_rows, num_slots, head_dim) for c in (k_heads, v_heads))

        def exchange(packed, lo):
            return {k: (lo, swap(block, k)) for k, block in packed.items()}

        def packed(caches, lo, hi, partners, group=1):
            return dict(zip(partners, pack_blocks(scalars, caches, (lo, hi), partners, group)))

        def swap_small(values):
            got = {k: swap(values[k], k) for k in near + far}
            return [values[0]] + [got[k] for k in range(1, N_DEV)]

        def chosen(*parts):
            merged = {k: v for part in parts for k, v in part.items()}
            return [merged[k] for k in range(1, N_DEV)]

        far_first = {}
        for k in far:
            blocks = {k: pack_first(start_pos, own, FIRST, k)}
            far_first.update(exchange(blocks, 0))
        positions = my_pos[None, :] + jnp.arange(n_steps)[:, None]
        queries, keys_new, values_new = project(hidden_in, positions, attn_norm, w_q, w_k, w_v, q_norm, k_norm)
        q_rows = jnp.transpose(queries.reshape(n_steps, num_rows, N_DEV, -1, head_dim), (1, 2, 0, 3, 4)).reshape(num_rows, N_DEV, -1, head_dim)
        k_rows = jnp.transpose(keys_new, (1, 2, 0, 3))
        v_rows = jnp.transpose(values_new, (1, 2, 0, 3))
        pack = jnp.concatenate([q_rows, k_rows, v_rows], axis=2)
        new = jnp.swapaxes(keys_new, 0, 1), jnp.swapaxes(values_new, 0, 1)
        pack_r = jnp.take(jnp.swapaxes(pack[LOCAL:], 0, 1), xor_heads, axis=0)
        got_q = swap_small([pack_r[k] for k in range(N_DEV)])
        near_blocks = packed(own, 0, LOCAL, near)
        middle_blocks = packed(own, FIRST, MIDDLE, far)
        local_blocks = packed(own, MIDDLE, LOCAL, far)
        near_local = exchange(near_blocks, 0)
        far_middle = exchange(middle_blocks, FIRST)
        far_local = {}
        for k in far:
            far_local.update(exchange({k: local_blocks[k]}, MIDDLE))
        o_r = remote_attend(scalars, own, got_q, LOCAL)
        got_o = swap_small(o_r)
        near_blocks = packed(own, LOCAL, num_rows, near)
        rest_blocks = packed(own, LOCAL, LAST, far)
        last_blocks = packed(own, LAST, num_rows, far)
        near_rest = exchange(near_blocks, LOCAL)
        far_last = exchange({far[0]: last_blocks[far[0]]}, LAST)
        far_rest = exchange(rest_blocks, LOCAL)
        far_last.update(exchange({k: last_blocks[k] for k in far[1:]}, LAST))
        *caches, o_a = settle(scalars, own, chosen(near_local, far_first), *new, pack, None, (0, FIRST), num_rows)
        *caches, o_b = settle(scalars, own, chosen(near_local, far_middle), *new, pack, caches, (FIRST, MIDDLE), num_rows)
        *caches, o_c = settle(scalars, own, chosen(near_local, far_local), *new, pack, caches, (MIDDLE, LOCAL), num_rows)
        attended = merge(scalars, (o_a, o_b, o_c), got_o).reshape(num_rows, N_DEV, n_steps, -1, head_dim)
        attended = jnp.transpose(attended, (2, 0, 1, 3, 4)).reshape(n_steps, num_rows, -1)
        out_hidden = finish(hidden_in, attended, w_o, mlp_norm, w_gate, w_up, w_down)
        caches = settle(scalars, own, chosen(near_rest, far_rest), *new, None, caches, (LOCAL, LAST), num_rows)
        caches = settle_last(start_pos, own, chosen(near_rest, far_last), *new, caches, LAST)
        return out_hidden, *caches

    return jax.shard_map(local_run, mesh=mesh, in_specs=(P('dp'), row_spec, cache_in, cache_in) + (P(),) * 11, out_specs=(row_spec, cache_out, cache_out), check_vma=False)
```
